16 devices in a mesh: req: 2 (over y, z), dap: 8 (over x, core).
Axes of the slice: x: 4, y: 2, z: 1, core: 2. Of those that a mesh axis runs over, the one named last changes fastest.
The devices are a block of a 4x4x8 slice.
Arguments:
- msa_act: bfloat16 [512, 256, 256], P(('req', 'dap')), parts along dimension 0
- pair_act: bfloat16 [512, 256, 128], P(('req', 'dap')), parts along dimension 0
- msa_mask: int32 [512, 256], P(('req', 'dap')), parts along dimension 0
- pair_mask: int32 [512, 256], P(('req', 'dap')), parts along dimension 0
- row_qkvg: bfloat16 [2, 256, 1024], replicated
- row_bias: bfloat16 [2, 128, 8], replicated
- row_out: bfloat16 [2, 256, 256], replicated
- col_qkvg: bfloat16 [2, 256, 1024], replicated
- col_out: bfloat16 [2, 256, 256], replicated
- mtr_in: bfloat16 [2, 256, 1024], replicated
- mtr_out: bfloat16 [2, 1024, 256], replicated
- opm_proj: bfloat16 [2, 256, 64], replicated
- opm_out: bfloat16 [2, 1024, 128], replicated
- tmo_proj: bfloat16 [2, 128, 640], replicated
- tmo_out: bfloat16 [2, 128, 128], replicated
- tmi_proj: bfloat16 [2, 128, 640], replicated
- tmi_out: bfloat16 [2, 128, 128], replicated
- tas_qkvg: bfloat16 [2, 128, 512], replicated
- tas_bias: bfloat16 [2, 128, 4], replicated
- tas_out: bfloat16 [2, 128, 128], replicated
- tae_qkvg: bfloat16 [2, 128, 512], replicated
- tae_bias: bfloat16 [2, 128, 4], replicated
- tae_out: bfloat16 [2, 128, 128], replicated
- ptr_in: bfloat16 [2, 128, 512], replicated
- ptr_out: bfloat16 [2, 512, 128], replicated
Outputs:
- output 1: bfloat16 [512, 256, 256], P(('req', 'dap')), parts along dimension 0
- output 2: bfloat16 [512, 256, 128], P(('req', 'dap')), parts along dimension 0
There are 2 independent parts. The reference program is written for one: setup_inputs(seed, part) draws one part's arguments, and reference() takes and returns one part's arrays. A program takes and returns all parts, laid end to end along the dimension named above; an argument that names none is the same for every part.
All inputs are finite; a program needn't handle non-finite values.
Results may differ from the reference program's by a relative error of at most 0.02.
Values are sent between devices in bfloat16 or wider.
A program may use at most 768 MiB of HBM per device.

```python
import jax
import jax.numpy as jnp
from jax import lax

SEQ = 256
RES = 256
MSA_DIM = 256
PAIR_DIM = 128
MSA_HEADS = 8
MSA_HEAD_DIM = 32
PAIR_HEADS = 4
PAIR_HEAD_DIM = 32
OPM_DIM = 32
TRI_DIM = 128
LAYERS = 2

WEIGHT_NAMES = ('row_qkvg', 'row_bias', 'row_out', 'col_qkvg', 'col_out', 'mtr_in', 'mtr_out', 'opm_proj', 'opm_out', 'tmo_proj', 'tmo_out', 'tmi_proj', 'tmi_out', 'tas_qkvg', 'tas_bias', 'tas_out', 'tae_qkvg', 'tae_bias', 'tae_out', 'ptr_in', 'ptr_out')


def weight_fans():
    msa_width = MSA_HEADS * MSA_HEAD_DIM
    pair_width = PAIR_HEADS * PAIR_HEAD_DIM
    return ((MSA_DIM, 4 * msa_width), (PAIR_DIM, MSA_HEADS), (msa_width, MSA_DIM),
            (MSA_DIM, 4 * msa_width), (msa_width, MSA_DIM),
            (MSA_DIM, 4 * MSA_DIM), (4 * MSA_DIM, MSA_DIM),
            (MSA_DIM, 2 * OPM_DIM), (OPM_DIM * OPM_DIM, PAIR_DIM),
            (PAIR_DIM, 4 * TRI_DIM + PAIR_DIM), (TRI_DIM, PAIR_DIM),
            (PAIR_DIM, 4 * TRI_DIM + PAIR_DIM), (TRI_DIM, PAIR_DIM),
            (PAIR_DIM, 4 * pair_width), (PAIR_DIM, PAIR_HEADS), (pair_width, PAIR_DIM),
            (PAIR_DIM, 4 * pair_width), (PAIR_DIM, PAIR_HEADS), (pair_width, PAIR_DIM),
            (PAIR_DIM, 4 * PAIR_DIM), (4 * PAIR_DIM, PAIR_DIM))


def draw_masks(mask_key):
    key_list = jax.random.split(mask_key, 4)
    pad_len = jax.random.randint(key_list[0], (), 1, RES // 16 + 1)
    res_ids = jnp.arange(RES)
    seq_ids = jnp.arange(SEQ)[:, None]
    is_valid = res_ids < RES - pad_len
    shallow = jax.random.randint(key_list[1], (RES,), 0, 4) == 0
    depths = jnp.where(shallow, jax.random.randint(key_list[2], (RES,), 1, SEQ // 4 + 1), SEQ)
    kept_mask = (jax.random.randint(key_list[3], (SEQ, RES), 0, 8) != 0) | (seq_ids == 0)
    msa_mask = ((seq_ids < depths[None, :]) & kept_mask & is_valid[None, :]).astype(jnp.int32)
    pair_mask = (is_valid[:, None] & is_valid[None, :]).astype(jnp.int32)
    return msa_mask, pair_mask


def setup_inputs(seed: int = 0, part: int = 0) -> dict:
    part_key = jax.random.fold_in(jax.random.key(seed), part)
    key_list = jax.random.split(part_key, 3)
    shared = jax.random.normal(key_list[0], (1, RES, MSA_DIM), jnp.float32)
    spread = jax.random.normal(key_list[1], (SEQ, RES, MSA_DIM), jnp.float32)
    msa_act = (shared + spread).astype(jnp.bfloat16)
    pair_act = jax.random.normal(key_list[2], (RES, RES, PAIR_DIM), jnp.float32).astype(jnp.bfloat16)
    msa_mask, pair_mask = draw_masks(jax.random.fold_in(part_key, 5))
    inputs = {'msa_act': msa_act, 'pair_act': pair_act, 'msa_mask': msa_mask, 'pair_mask': pair_mask}
    weight_key = jax.random.key(seed + 1)
    for w_index, fan_pair in enumerate(weight_fans()):
        sample = jax.random.normal(jax.random.fold_in(weight_key, w_index), (LAYERS,) + fan_pair, jnp.float32)
        inputs[WEIGHT_NAMES[w_index]] = (sample * fan_pair[0] ** -0.5).astype(jnp.bfloat16)
    return inputs


def layer_norm(x):
    values = x.astype(jnp.float32)
    centered = values - jnp.mean(values, axis=-1, keepdims=True)
    variance = jnp.mean(centered * centered, axis=-1, keepdims=True)
    return (centered * lax.rsqrt(variance + 1e-5)).astype(jnp.bfloat16)


def linear(x, weight):
    flat_x = x.reshape(-1, x.shape[-1])
    result = jnp.dot(flat_x, weight, preferred_element_type=jnp.float32)
    return result.reshape(x.shape[:-1] + (weight.shape[-1],))


def residual(x, update):
    return (x.astype(jnp.float32) + update).astype(jnp.bfloat16)


def attend_row(x_row, bias_hij, mask_row, w_qkvg, w_out, num_heads):
    length = x_row.shape[0]
    head_width = w_out.shape[0]
    head_dim = head_width // num_heads
    projected = jnp.dot(x_row, w_qkvg, preferred_element_type=jnp.float32).astype(jnp.bfloat16).astype(jnp.float32)
    queries = projected[:, :head_width].reshape(length, num_heads, head_dim)
    keyset = projected[:, head_width:2 * head_width].reshape(length, num_heads, head_dim)
    valset = projected[:, 2 * head_width:3 * head_width].reshape(length, num_heads, head_dim)
    gate_act = jax.nn.sigmoid(projected[:, 3 * head_width:])
    logits = jnp.einsum('ihd,jhd->hij', queries, keyset) * head_dim ** -0.5 + bias_hij.astype(jnp.float32)
    logits = jnp.where(mask_row[None, None, :] > 0, logits, -1e9)
    attn_prob = jax.nn.softmax(logits, axis=-1).astype(jnp.bfloat16).astype(jnp.float32)
    attended = jnp.einsum('hij,jhd->ihd', attn_prob, valset).reshape(length, head_width)
    gated = (attended * gate_act).astype(jnp.bfloat16)
    return jnp.dot(gated, w_out, preferred_element_type=jnp.float32)


def row_attention(msa_act, pair_act, msa_mask, w_qkvg, w_bias, w_out):
    pair_bias = jnp.transpose(linear(layer_norm(pair_act), w_bias).astype(jnp.bfloat16), (2, 0, 1))
    msa_norm = layer_norm(msa_act)
    return lax.map(lambda item: attend_row(item[0], pair_bias, item[1], w_qkvg, w_out, w_bias.shape[1]), (msa_norm, msa_mask))


def column_attention(msa_act, msa_mask, w_qkvg, w_out, num_heads):
    msa_norm = jnp.swapaxes(layer_norm(msa_act), 0, 1)
    zero_bias = jnp.zeros((1, 1, 1), jnp.float32)
    update = lax.map(lambda item: attend_row(item[0], zero_bias, item[1], w_qkvg, w_out, num_heads), (msa_norm, msa_mask.T))
    return jnp.swapaxes(update, 0, 1)


def transition(x, w_in, w_out):
    hidden = jnp.maximum(linear(layer_norm(x), w_in), 0.0).astype(jnp.bfloat16)
    return linear(hidden, w_out)


def outer_product_mean(msa_act, msa_mask, w_proj, w_out):
    opm_dim = w_proj.shape[1] // 2
    projected = linear(layer_norm(msa_act), w_proj).astype(jnp.bfloat16)
    mask_bf = msa_mask.astype(jnp.bfloat16)[:, :, None]
    left_act = (projected[..., :opm_dim] * mask_bf).astype(jnp.float32)
    right_act = (projected[..., opm_dim:] * mask_bf).astype(jnp.float32)
    mask_f = msa_mask.astype(jnp.float32)
    overlap = jnp.dot(mask_f.T, mask_f)

    def outer_row(left_row):
        outer_prod = jnp.einsum('sc,sje->jce', left_row, right_act).astype(jnp.bfloat16)
        return linear(outer_prod.reshape(outer_prod.shape[0], opm_dim * opm_dim), w_out)

    update = lax.map(outer_row, jnp.swapaxes(left_act, 0, 1))
    return update / (1e-3 + overlap)[:, :, None]


def tri_mul(pair_act, pair_mask, w_proj, w_out, form):
    tri_dim = (w_proj.shape[1] - pair_act.shape[-1]) // 4
    projected = linear(layer_norm(pair_act), w_proj)
    mask_f = pair_mask.astype(jnp.float32)[:, :, None]
    left_act = (mask_f * jax.nn.sigmoid(projected[..., 2 * tri_dim:3 * tri_dim]) * projected[..., :tri_dim]).astype(jnp.bfloat16)
    right_act = (mask_f * jax.nn.sigmoid(projected[..., 3 * tri_dim:4 * tri_dim]) * projected[..., tri_dim:2 * tri_dim]).astype(jnp.bfloat16)
    gate_act = jax.nn.sigmoid(projected[..., 4 * tri_dim:])
    product = jnp.einsum(form, left_act.astype(jnp.float32), right_act.astype(jnp.float32))
    return gate_act * linear(layer_norm(product), w_out)


def tri_attention(pair_act, pair_mask, w_qkvg, w_bias, w_out):
    pair_norm = layer_norm(pair_act)
    pair_bias = jnp.transpose(linear(pair_norm, w_bias).astype(jnp.bfloat16), (2, 0, 1))
    return lax.map(lambda item: attend_row(item[0], pair_bias, item[1], w_qkvg, w_out, w_bias.shape[1]), (pair_norm, pair_mask))


def evoformer_block(msa_act, pair_act, msa_mask, pair_mask, layer_w):
    (row_qkvg, row_bias, row_out, col_qkvg, col_out, mtr_in, mtr_out, opm_proj, opm_out,
     tmo_proj, tmo_out, tmi_proj, tmi_out, tas_qkvg, tas_bias, tas_out,
     tae_qkvg, tae_bias, tae_out, ptr_in, ptr_out) = layer_w
    msa_act = residual(msa_act, row_attention(msa_act, pair_act, msa_mask, row_qkvg, row_bias, row_out))
    msa_act = residual(msa_act, column_attention(msa_act, msa_mask, col_qkvg, col_out, row_bias.shape[1]))
    msa_act = residual(msa_act, transition(msa_act, mtr_in, mtr_out))
    pair_act = residual(pair_act, outer_product_mean(msa_act, msa_mask, opm_proj, opm_out))
    pair_act = residual(pair_act, tri_mul(pair_act, pair_mask, tmo_proj, tmo_out, 'ikc,jkc->ijc'))
    pair_act = residual(pair_act, tri_mul(pair_act, pair_mask, tmi_proj, tmi_out, 'kic,kjc->ijc'))
    pair_act = residual(pair_act, tri_attention(pair_act, pair_mask, tas_qkvg, tas_bias, tas_out))
    pair_swap = jnp.swapaxes(pair_act, 0, 1)
    pair_act = residual(pair_act, jnp.swapaxes(tri_attention(pair_swap, pair_mask.T, tae_qkvg, tae_bias, tae_out), 0, 1))
    pair_act = residual(pair_act, transition(pair_act, ptr_in, ptr_out))
    return msa_act, pair_act


def reference(msa_act, pair_act, msa_mask, pair_mask, row_qkvg, row_bias, row_out, col_qkvg, col_out, mtr_in, mtr_out, opm_proj, opm_out, tmo_proj, tmo_out, tmi_proj, tmi_out, tas_qkvg, tas_bias, tas_out, tae_qkvg, tae_bias, tae_out, ptr_in, ptr_out):
    stacked = (row_qkvg, row_bias, row_out, col_qkvg, col_out, mtr_in, mtr_out, opm_proj, opm_out,
               tmo_proj, tmo_out, tmi_proj, tmi_out, tas_qkvg, tas_bias, tas_out,
               tae_qkvg, tae_bias, tae_out, ptr_in, ptr_out)

    def step(carry, layer_w):
        return evoformer_block(carry[0], carry[1], msa_mask, pair_mask, layer_w), None

    carried, ignored = lax.scan(step, (msa_act, pair_act), stacked)
    return carried[0], carried[1]
```

```python
import functools
import math

import jax
import jax.numpy as jnp
from jax import lax
from jax.experimental import pallas as pl
from jax.experimental.pallas import tpu as pltpu
from jax.sharding import PartitionSpec as P

GROUP_AXIS = 'dap'
PARTS_AXIS = 'req'
LOG2E = math.log2(math.e)
MASKED = -1e9 * LOG2E
F32, BF16 = jnp.float32, jnp.bfloat16
VMEM_LIMIT = 60 * 1024 * 1024


def nn(a, b):
    return lax.dot_general(a, b, (((1,), (0,)), ((), ())), preferred_element_type=F32)


def nt(a, b):
    return lax.dot_general(a, b, (((1,), (1,)), ((), ())), preferred_element_type=F32)


def tn(a, b):
    return lax.dot_general(a, b, (((0,), (0,)), ((), ())), preferred_element_type=F32)


def norm(x):
    centered = x - jnp.mean(x, axis=-1, keepdims=True)
    variance = jnp.mean(centered * centered, axis=-1, keepdims=True)
    return (centered * lax.rsqrt(variance + 1e-5)).astype(BF16)


def flip(w):
    return w.astype(F32).T.astype(w.dtype)


def key_column(mask_row):
    return jnp.broadcast_to(mask_row, (128, mask_row.shape[1])).T


def project_row(r, x_norm, mask_row, wt_ref, proj_s, keep_s):
    proj_s[r] = nt(wt_ref[...], x_norm).astype(BF16)
    keep_s[r] = key_column(mask_row)


def attend_row(r, proj_s, keep_s, gated_s, bias_ref, heads):
    width, length = gated_s.shape[1:]
    dim = width // heads
    column = keep_s[r]
    kept = jnp.concatenate([column] * (length // 128), axis=1) > 0

    def part(n, h):
        return proj_s[r, n * width + h * dim:n * width + (h + 1) * dim, :]

    def scores(h):
        logits = tn(part(1, h), part(0, h)) * (dim ** -0.5 * LOG2E)
        if bias_ref is not None:
            logits = logits + bias_ref[h]
        return jnp.where(kept, logits, MASKED)

    def weigh(logits):
        expd = jnp.exp2(logits - jnp.max(logits, axis=0, keepdims=True))
        return (expd * (1.0 / jnp.sum(expd, axis=0, keepdims=True))).astype(BF16)

    def gate(h, probs):
        gated = nn(part(2, h), probs) * jax.nn.sigmoid(part(3, h).astype(F32))
        gated_s[r, h * dim:(h + 1) * dim, :] = gated.astype(BF16)

    probs = None
    ahead = scores(0)
    for h in range(heads):
        logits, ahead = ahead, scores(h + 1) if h + 1 < heads else None
        if probs is not None:
            gate(h - 1, probs)
        probs = weigh(logits)
    gate(heads - 1, probs)


def attend_rows(rows, proj_s, keep_s, gated_s, bias_ref, heads):
    def body(r, carry):
        attend_row(r, proj_s, keep_s, gated_s, bias_ref, heads)
        return carry
    lax.fori_loop(0, rows, body, 0)


def attention_scratch(rows, length, w, w_out):
    return [pltpu.VMEM((rows, w.shape[1], length), BF16), pltpu.VMEM((rows, length, 128), F32),
            pltpu.VMEM((rows, w_out.shape[0], length), BF16)]


def each(count, body, unroll=1):
    def step(n, carry):
        body(n)
        return carry
    lax.fori_loop(0, count, step, 0, unroll=unroll)


def load_bias(bias_ref, bias_s, transposed):
    for h in range(bias_s.shape[0]):
        bias = bias_ref[h].astype(F32) * LOG2E
        bias_s[h] = bias.T if transposed else bias


def transition(x, w_in_ref, w_out_ref):
    hidden = jnp.maximum(nn(norm(x), w_in_ref[...]), 0.0).astype(BF16)
    return nn(hidden, w_out_ref[...])


def residual(x, update):
    total = (x + update).astype(BF16)
    return total, total.astype(F32)


def rows_of(ref, start, count, step):
    return ref[pl.ds(start, count, stride=step), :]


def call(kernel, grid, in_specs, out_specs, out_shape, scratch, flops):
    return pl.pallas_call(
        kernel, grid=grid, in_specs=in_specs, out_specs=out_specs, out_shape=out_shape, scratch_shapes=scratch,
        compiler_params=pltpu.CompilerParams(vmem_limit_bytes=VMEM_LIMIT),
        cost_estimate=pl.CostEstimate(flops=flops, bytes_accessed=1 << 24, transcendentals=0))


def full_spec(array):
    zeros = (0,) * array.ndim
    return pl.BlockSpec(array.shape, lambda n: zeros)


def lead_spec(block, axis):
    return pl.BlockSpec(block, lambda n: tuple(n if d == axis else 0 for d in range(len(block))))


def bias_rows(store, n, x_norm, wbt_ref):
    values = nt(wbt_ref[...], x_norm)
    for t in range(store.shape[0]):
        store[t, pl.ds(pl.multiple_of(n * 8, 8), 8), :] = values[:, t * 128:(t + 1) * 128]


def bias_scratch(rows, length):
    return pltpu.VMEM((length // 128, rows * 8, 128), F32)


def write_bias(out_ref, store, rows):
    for h in range(out_ref.shape[0]):
        out_ref[h] = take_row(store, h, rows, 8).astype(BF16)


def bias_kernel(z_ref, wbt_ref, out_ref, store):
    rows = z_ref.shape[0]

    def body(n, carry):
        bias_rows(store, n, norm(z_ref[n].astype(F32)), wbt_ref)
        return carry
    lax.fori_loop(0, rows, body, 0)
    write_bias(out_ref, store, rows)


def pair_bias(z, wbt, heads):
    rows, length, _ = z.shape
    return call(bias_kernel, (1,), [full_spec(z), full_spec(wbt)], lead_spec((heads, rows, length), 1),
                jax.ShapeDtypeStruct((heads, rows, length), BF16), [bias_scratch(rows, length)], 10 ** 8)(z, wbt)


def row_kernel(transposed, heads, m_ref, mask_ref, bias_ref, w_ref, w_out_ref, out_ref, bias_s, wt_s, proj_s, keep_s, gated_s):
    rows = m_ref.shape[0]

    @pl.when(pl.program_id(0) == 0)
    def _():
        load_bias(bias_ref, bias_s, transposed)
        wt_s[...] = flip(w_ref[...])

    def project(s):
        project_row(s, norm(m_ref[s].astype(F32)), mask_ref[pl.ds(s, 1), :], wt_s, proj_s, keep_s)
    each(rows, project, 2)
    attend_rows(rows, proj_s, keep_s, gated_s, bias_s, heads)

    def finish(s):
        out_ref[s] = residual(m_ref[s].astype(F32), tn(gated_s[s], w_out_ref[...]))[0]
    each(rows, finish, 2)


def row_attention(m, mask, bias, transposed, w, w_out):
    seqs, length, chans = m.shape
    heads = bias.shape[0]
    block = 8
    return call(functools.partial(row_kernel, transposed, heads), (seqs // block,),
                [lead_spec((block, length, chans), 0), lead_spec((block, length), 0), full_spec(bias), full_spec(w), full_spec(w_out)],
                lead_spec((block, length, chans), 0), jax.ShapeDtypeStruct(m.shape, BF16),
                [pltpu.VMEM((heads, length, length), F32), pltpu.VMEM(w.shape[::-1], BF16)] + attention_scratch(block, length, w, w_out),
                2 * 10 ** 10)(m, mask, bias, w, w_out)


def split_store(dst, x):
    seqs, rows, chans = x.shape
    flat = x.astype(F32).reshape(seqs * rows, chans)
    for t in range(chans // 128):
        dst[t] = flat[:, t * 128:(t + 1) * 128]


def take_row(src, r, count, step):
    return jnp.concatenate([src[t, pl.ds(r, count, stride=step), :] for t in range(src.shape[0])], axis=1)


def put_row(dst, r, count, step, value):
    for t in range(dst.shape[0]):
        dst[t, pl.ds(r, count, stride=step), :] = value[:, t * 128:(t + 1) * 128]


def join_store(src, shape):
    seqs, rows, chans = shape
    return jnp.concatenate([src[t] for t in range(src.shape[0])], axis=1).reshape(seqs, rows, chans).astype(BF16)


def col_kernel(heads, m_ref, mask_ref, w_ref, w_out_ref, tin_ref, tout_ref, op_ref, out_ref, a_ref, b_ref, x_s, b_s, wt_s, opt_s, proj_s, keep_s, gated_s):
    seqs, rows, chans = m_ref.shape
    dim = op_ref.shape[1] // 2

    @pl.when(pl.program_id(0) == 0)
    def _():
        wt_s[...] = flip(w_ref[...])
        opt_s[...] = flip(op_ref[...])
    split_store(x_s, m_ref[...])

    def project(r):
        project_row(r, norm(take_row(x_s, r, seqs, rows)), mask_ref[pl.ds(r, 1), :], wt_s, proj_s, keep_s)
    each(rows, project, 2)
    attend_rows(rows, proj_s, keep_s, gated_s, None, heads)

    def finish(r):
        mask_row = mask_ref[pl.ds(r, 1), :]
        x = take_row(x_s, r, seqs, rows)
        x = residual(x, tn(gated_s[r], w_out_ref[...]))[1]
        x = residual(x, transition(x, tin_ref, tout_ref))[1]
        put_row(x_s, r, seqs, rows, x)
        proj = nt(opt_s[...], norm(x)).astype(BF16).astype(F32) * mask_row
        a_ref[r] = proj[:dim].astype(BF16)
        for t in range(seqs // 128):
            b_s[t, pl.ds(r, dim, stride=rows), :] = proj[dim:, t * 128:(t + 1) * 128]
    each(rows, finish)
    out_ref[...] = join_store(x_s, m_ref.shape)
    b_ref[...] = join_store(b_s, b_ref.shape)


def column_block(m, mask_t, heads, w, w_out, t_in, t_out, o_proj):
    seqs, rows, chans = m.shape
    dim = o_proj.shape[1] // 2
    block = 16
    weights = (w, w_out, t_in, t_out, o_proj)
    return call(functools.partial(col_kernel, heads), (rows // block,),
                [lead_spec((seqs, block, chans), 1), lead_spec((block, seqs), 0)] + [full_spec(x) for x in weights],
                [lead_spec((seqs, block, chans), 1), lead_spec((block, dim, seqs), 0), lead_spec((dim, block, seqs), 1)],
                [jax.ShapeDtypeStruct(m.shape, BF16), jax.ShapeDtypeStruct((rows, dim, seqs), BF16), jax.ShapeDtypeStruct((dim, rows, seqs), BF16)],
                [pltpu.VMEM((chans // 128, seqs * block, 128), F32), pltpu.VMEM((seqs // 128, dim * block, 128), F32),
                 pltpu.VMEM(w.shape[::-1], BF16), pltpu.VMEM(o_proj.shape[::-1], BF16)] + attention_scratch(block, seqs, w, w_out),
                3 * 10 ** 10)(m, mask_t, *weights)


def gate_parts(z_norm, mask_row, wt_ref, tri):
    proj = nt(wt_ref[pl.ds(0, 4 * tri), :], z_norm)
    left = mask_row * jax.nn.sigmoid(proj[2 * tri:3 * tri]) * proj[:tri]
    right = mask_row * jax.nn.sigmoid(proj[3 * tri:]) * proj[tri:2 * tri]
    return left, right


def put_channels(dst, n, step, value):
    for t in range(dst.shape[0]):
        dst[t, pl.ds(n, value.shape[0], stride=step), :] = value[:, t * 128:(t + 1) * 128]


def opm_kernel(a_ref, b_ref, z_ref, rmask_ref, fmask_ref, pmask_ref, w_ref, proj_ref,
               z_out, l_out, r_out, wf_s, wt_s, gt_s, o_s, scale_s, l_s, r_s):
    rows, dim, seqs = a_ref.shape
    tri = l_out.shape[0]

    @pl.when(pl.program_id(0) == 0)
    def _():
        gt_s[...] = flip(proj_ref[...])
        wf_s[...] = w_ref[...].astype(F32)
        swapped = [rows_of(wf_s, e, dim, dim) for e in range(dim)]
        wt_s[...] = jnp.concatenate(swapped, axis=0).T.astype(BF16)
    scale_s[...] = 1.0 / (1e-3 + nt(rmask_ref[...].astype(BF16), fmask_ref[...].astype(BF16)))

    def outer(e, carry):
        prod = nt(a_ref[...].reshape(rows * dim, seqs), b_ref[e]).astype(BF16)
        for i in range(rows):
            o_s[i, pl.ds(pl.multiple_of(e * dim, dim), dim), :] = prod[i * dim:(i + 1) * dim]
        return carry
    lax.fori_loop(0, dim, outer, 0, unroll=2)

    def finish(i, carry):
        update = (nn(wt_s[...], o_s[i]) * scale_s[pl.ds(i, 1), :]).T
        total, total_f = residual(z_ref[i].astype(F32), update)
        z_out[i] = total
        left, right = gate_parts(norm(total_f), pmask_ref[pl.ds(i, 1), :], gt_s, tri)
        put_channels(l_s, i, rows, left)
        put_channels(r_s, i, rows, right)
        return carry
    lax.fori_loop(0, rows, finish, 0)
    l_out[...] = join_store(l_s, l_out.shape)
    r_out[...] = join_store(r_s, r_out.shape)


def outer_block(a, b_full, z, rmask, fmask, pmask, w_out, tri_proj):
    rows, dim, seqs = a.shape
    length, out_dim = z.shape[1:]
    tri = (tri_proj.shape[1] - out_dim) // 4
    block = 16
    consts = (w_out, tri_proj)
    chan_shape = jax.ShapeDtypeStruct((tri, rows, length), BF16)
    chan_scratch = pltpu.VMEM((length // 128, tri * block, 128), F32)
    return call(opm_kernel, (rows // block,),
                [lead_spec((block, dim, seqs), 0), full_spec(b_full), lead_spec((block, length, out_dim), 0), lead_spec((block, seqs), 0),
                 full_spec(fmask), lead_spec((block, length), 0)] + [full_spec(x) for x in consts],
                [lead_spec((block, length, out_dim), 0), lead_spec((tri, block, length), 1), lead_spec((tri, block, length), 1)],
                [jax.ShapeDtypeStruct(z.shape, BF16), chan_shape, chan_shape],
                [pltpu.VMEM(w_out.shape, F32), pltpu.VMEM(w_out.shape[::-1], BF16), pltpu.VMEM(tri_proj.shape[::-1], BF16),
                 pltpu.VMEM((block, dim * dim, length), BF16), pltpu.VMEM((block, length), F32), chan_scratch, chan_scratch],
                10 ** 10)(a, b_full, z, rmask, fmask, pmask, *consts)


def put_product(x_s, c, rows, prod):
    for t in range(x_s.shape[0]):
        x_s[t, pl.ds(pl.multiple_of(c * rows, rows), rows), :] = prod[:, t * 128:(t + 1) * 128]


def tri_finish(x_s, z, i, rows, proj_ref, w_out_ref):
    out_dim = z.shape[1]
    chans = w_out_ref.shape[0]
    x = take_row(x_s, i, chans, rows)
    centered = x - jnp.mean(x, axis=0, keepdims=True)
    variance = jnp.mean(centered * centered, axis=0, keepdims=True)
    x_norm = (centered * lax.rsqrt(variance + 1e-5)).astype(BF16)
    gate = jax.nn.sigmoid(nn(norm(z), proj_ref[:, 4 * chans:4 * chans + out_dim]))
    return residual(z, gate * tn(x_norm, w_out_ref[...]))


def outgoing_kernel(a_ref, b_ref, z_ref, pmask_ref, proj_ref, w_out_ref, next_ref, z_out, l_out, r_out, x_s, r_s, gt_s):
    step, steps = pl.program_id(0), pl.num_programs(0)
    block, rows, _ = a_ref.shape
    tri = w_out_ref.shape[0]

    def product(c, carry):
        put_product(x_s, step * block + c, rows, nt(a_ref[c], b_ref[c]))
        return carry
    lax.fori_loop(0, block, product, 0, unroll=4)

    @pl.when(step == steps - 1)
    def _():
        gt_s[...] = flip(next_ref[...])

        def finish(i, carry):
            total, total_f = tri_finish(x_s, z_ref[i].astype(F32), i, rows, proj_ref, w_out_ref)
            z_out[i] = total
            z_norm = norm(total_f)
            mask_row = pmask_ref[pl.ds(i, 1), :]
            value = nn(z_norm, next_ref[:, :tri])
            value_gate = nn(z_norm, next_ref[:, 2 * tri:3 * tri])
            l_out[i] = (key_column(mask_row) * jax.nn.sigmoid(value_gate) * value).astype(BF16)
            right = nt(gt_s[pl.ds(tri, tri), :], z_norm)
            right_gate = nt(gt_s[pl.ds(3 * tri, tri), :], z_norm)
            put_channels(r_s, i, rows, mask_row * jax.nn.sigmoid(right_gate) * right)
            return carry
        lax.fori_loop(0, rows, finish, 0)
        r_out[...] = join_store(r_s, r_out.shape)


def outgoing(a, b_full, z, pmask, proj, w_out, next_proj):
    tri, rows, length = a.shape
    block = 16
    consts = (z, pmask, proj, w_out, next_proj)
    scratch = pltpu.VMEM((length // 128, tri * rows, 128), F32)
    outs = [jax.ShapeDtypeStruct(z.shape, BF16), jax.ShapeDtypeStruct((rows, length, tri), BF16), jax.ShapeDtypeStruct((tri, rows, length), BF16)]
    return call(outgoing_kernel, (tri // block,),
                [lead_spec((block, rows, length), 0), lead_spec((block, length, length), 0)] + [full_spec(x) for x in consts],
                [full_spec(x) for x in outs], outs, [scratch, scratch, pltpu.VMEM(next_proj.shape[::-1], BF16)], 10 ** 10)(a, b_full, *consts)


def incoming_kernel(a_ref, b_ref, z_ref, proj_ref, w_out_ref, wbt_ref, z_out, bias_out, af_s, a_s, x_s, bias_s):
    step, steps = pl.program_id(0), pl.num_programs(0)
    block = b_ref.shape[0]
    length, rows, tri = a_ref.shape

    @pl.when(step == 0)
    def _():
        af_s[...] = a_ref[...].astype(F32).reshape(length * rows, tri)

        def turn(i, carry):
            put_channels(a_s, i, rows, rows_of(af_s, i, length, rows).T)
            return carry
        lax.fori_loop(0, rows, turn, 0)

    def product(c, carry):
        place = pl.ds(pl.multiple_of((step * block + c) * rows, rows), rows)
        left = jnp.concatenate([a_s[t, place, :] for t in range(a_s.shape[0])], axis=1).astype(BF16)
        put_product(x_s, step * block + c, rows, nn(left, b_ref[c]))
        return carry
    lax.fori_loop(0, block, product, 0, unroll=4)

    @pl.when(step == steps - 1)
    def _():
        def finish(i, carry):
            total, total_f = tri_finish(x_s, z_ref[i].astype(F32), i, rows, proj_ref, w_out_ref)
            z_out[i] = total
            bias_rows(bias_s, i, norm(total_f), wbt_ref)
            return carry
        lax.fori_loop(0, rows, finish, 0)
        write_bias(bias_out, bias_s, rows)


def incoming(a, b_full, z, proj, w_out, wbt, heads):
    length, rows, tri = a.shape
    block = 16
    consts = (z, proj, w_out, wbt)
    scratch = pltpu.VMEM((length // 128, tri * rows, 128), F32)
    outs = [jax.ShapeDtypeStruct(z.shape, BF16), jax.ShapeDtypeStruct((heads, rows, length), BF16)]
    return call(incoming_kernel, (tri // block,),
                [full_spec(a), lead_spec((block, length, length), 0)] + [full_spec(x) for x in consts],
                [full_spec(x) for x in outs], outs,
                [pltpu.VMEM((length * rows, tri), F32), scratch, scratch, bias_scratch(rows, length)],
                10 ** 10)(a, b_full, *consts)


def start_kernel(heads, z_ref, mask_ref, bias_ref, w_ref, w_out_ref, wbt_ref, z_out, bias_out, bias_s, wt_s, next_s, proj_s, keep_s, gated_s):
    rows = z_ref.shape[0]

    @pl.when(pl.program_id(0) == 0)
    def _():
        load_bias(bias_ref, bias_s, True)
        wt_s[...] = flip(w_ref[...])

    def project(i):
        project_row(i, norm(z_ref[i].astype(F32)), mask_ref[pl.ds(i, 1), :], wt_s, proj_s, keep_s)
    each(rows, project, 4)
    attend_rows(rows, proj_s, keep_s, gated_s, bias_s, heads)

    def finish(i):
        total, total_f = residual(z_ref[i].astype(F32), tn(gated_s[i], w_out_ref[...]))
        z_out[i] = total
        bias_rows(next_s, i, norm(total_f), wbt_ref)
    each(rows, finish, 4)
    write_bias(bias_out, next_s, rows)


def start_attention(z, mask, bias, w, w_out, wbt):
    rows, length, chans = z.shape
    heads = bias.shape[0]
    block = 16
    consts = (bias, w, w_out, wbt)
    return call(functools.partial(start_kernel, heads), (rows // block,),
                [lead_spec((block, length, chans), 0), lead_spec((block, length), 0)] + [full_spec(x) for x in consts],
                [lead_spec((block, length, chans), 0), lead_spec((heads, block, length), 1)],
                [jax.ShapeDtypeStruct(z.shape, BF16), jax.ShapeDtypeStruct((heads, rows, length), BF16)],
                [pltpu.VMEM((heads, length, length), F32), pltpu.VMEM(w.shape[::-1], BF16), bias_scratch(block, length)]
                + attention_scratch(block, length, w, w_out), 10 ** 10)(z, mask, *consts)


def end_kernel(heads, z_ref, mask_ref, bias_ref, w_ref, w_out_ref, tin_ref, tout_ref, wbt_ref, z_out, bias_out, x_s, bias_s, wt_s, next_s, proj_s, keep_s, gated_s):
    length, cols, chans = z_ref.shape

    @pl.when(pl.program_id(0) == 0)
    def _():
        load_bias(bias_ref, bias_s, False)
        wt_s[...] = flip(w_ref[...])
    split_store(x_s, z_ref[...])

    def project(j):
        project_row(j, norm(take_row(x_s, j, length, cols)), mask_ref[pl.ds(j, 1), :], wt_s, proj_s, keep_s)
    each(cols, project, 4)
    attend_rows(cols, proj_s, keep_s, gated_s, bias_s, heads)

    def finish(j):
        x = take_row(x_s, j, length, cols)
        x = residual(x, tn(gated_s[j], w_out_ref[...]))[1]
        x = residual(x, transition(x, tin_ref, tout_ref))[1]
        put_row(x_s, j, length, cols, x)
        bias_rows(next_s, j, norm(x), wbt_ref)
    each(cols, finish, 2)
    z_out[...] = join_store(x_s, z_ref.shape)
    write_bias(bias_out, next_s, cols)


def end_attention(z, mask_t, bias, w, w_out, t_in, t_out, wbt, next_heads):
    length, cols, chans = z.shape
    heads = bias.shape[0]
    block = 16
    consts = (bias, w, w_out, t_in, t_out, wbt)
    return call(functools.partial(end_kernel, heads), (cols // block,),
                [lead_spec((length, block, chans), 1), lead_spec((block, length), 0)] + [full_spec(x) for x in consts],
                [lead_spec((length, block, chans), 1), lead_spec((next_heads, block, length), 1)],
                [jax.ShapeDtypeStruct(z.shape, BF16), jax.ShapeDtypeStruct((next_heads, cols, length), BF16)],
                [pltpu.VMEM((chans // 128, length * block, 128), F32), pltpu.VMEM((heads, length, length), F32),
                 pltpu.VMEM(w.shape[::-1], BF16), bias_scratch(block, length)] + attention_scratch(block, length, w, w_out),
                10 ** 10)(z, mask_t, *consts)


def gather(x, axis):
    return lax.all_gather(x, GROUP_AXIS, axis=axis, tiled=True)


def exchange(x, split, concat):
    return lax.all_to_all(x, GROUP_AXIS, split, concat, tiled=True)


def bias_weight(w):
    return jnp.pad(w.T, ((0, 8 - w.shape[1]), (0, 0)))


def solution(mesh):
    row_spec = P((PARTS_AXIS, GROUP_AXIS))

    def local_body(m, z, msa_mask, pair_mask, *weights):
        layers = weights[0].shape[0]
        seq_loc, res_loc = m.shape[0], z.shape[0]
        shard = lax.axis_index(GROUP_AXIS)
        heads = weights[1].shape[2]
        pair_heads = weights[14].shape[2]
        row_bias_w = [bias_weight(weights[1][n]) for n in range(layers)]
        seq_mask, row_mask = msa_mask.astype(F32), pair_mask.astype(F32)
        bias = pair_bias(z, row_bias_w[0], heads)
        packed = gather(jnp.concatenate([bias, msa_mask.astype(BF16)[None], pair_mask.astype(BF16)[None]]), 1)
        bias = packed[:heads]
        masks_t = jnp.swapaxes(packed[heads:].astype(F32), 1, 2)
        full_mask_t = masks_t[0]
        res_mask_t, col_mask = (lax.dynamic_slice_in_dim(x, shard * res_loc, res_loc, 0) for x in masks_t)
        for n in range(layers):
            (row_qkvg, _, row_out, col_qkvg, col_out, mtr_in, mtr_out, opm_proj, opm_out, tmo_proj, tmo_out, tmi_proj, tmi_out,
             tas_qkvg, tas_bias, tas_out, tae_qkvg, tae_bias, tae_out, ptr_in, ptr_out) = (weight[n] for weight in weights)
            m = row_attention(m, seq_mask, bias, n == 0, row_qkvg, row_out)
            m = exchange(m, 1, 0)
            m, left, right = column_block(m, res_mask_t, heads, col_qkvg, col_out, mtr_in, mtr_out, opm_proj)
            right = gather(right, 1)
            m = exchange(m, 0, 1)
            z, left, right = outer_block(left, right, z, res_mask_t, full_mask_t, row_mask, opm_out, tmo_proj)
            z, left, right = outgoing(left, gather(right, 1), z, row_mask, tmo_proj, tmo_out, tmi_proj)
            z, bias = incoming(exchange(left, 1, 0), gather(right, 1), z, tmi_proj, tmi_out, bias_weight(tas_bias), pair_heads)
            z, bias = start_attention(z, row_mask, gather(bias, 1), tas_qkvg, tas_out, bias_weight(tae_bias))
            bias = gather(bias, 1)
            z, bias = end_attention(exchange(z, 1, 0), col_mask, bias, tae_qkvg, tae_out, ptr_in, ptr_out,
                                    row_bias_w[min(n + 1, layers - 1)], heads)
            if n < layers - 1:
                bias = gather(bias, 1)
            z = exchange(z, 0, 1)
        return m, z

    def run_blocks(*arrays):
        n_weights = len(arrays) - 4
        return jax.shard_map(local_body, mesh=mesh, in_specs=(row_spec,) * 4 + (P(),) * n_weights, out_specs=(row_spec, row_spec), check_vma=False)(*arrays)

    return run_blocks
```

```python
import functools
import math

import jax
import jax.numpy as jnp
from jax import lax
from jax.experimental import pallas as pl
from jax.experimental.pallas import tpu as pltpu
from jax.sharding import PartitionSpec as P

GROUP_AXIS = 'dap'
PARTS_AXIS = 'req'
LOG2E = math.log2(math.e)
MASKED = -1e9 * LOG2E
F32, BF16 = jnp.float32, jnp.bfloat16
VMEM_LIMIT = 60 * 1024 * 1024


def nn(a, b):
    return lax.dot_general(a, b, (((1,), (0,)), ((), ())), preferred_element_type=F32)


def nt(a, b):
    return lax.dot_general(a, b, (((1,), (1,)), ((), ())), preferred_element_type=F32)


def tn(a, b):
    return lax.dot_general(a, b, (((0,), (0,)), ((), ())), preferred_element_type=F32)


def norm(x):
    centered = x - jnp.mean(x, axis=-1, keepdims=True)
    variance = jnp.mean(centered * centered, axis=-1, keepdims=True)
    return (centered * lax.rsqrt(variance + 1e-5)).astype(BF16)


def norm_steps(x):
    centered = x - jnp.mean(x, axis=-1, keepdims=True)
    yield
    variance = jnp.mean(centered * centered, axis=-1, keepdims=True)
    yield
    return (centered * lax.rsqrt(variance + 1e-5)).astype(BF16)


def together(count, body, group):
    def step(n, carry):
        live = [body(n * group + g) for g in range(group)]
        while live:
            going = []
            for member in live:
                try:
                    next(member)
                    going.append(member)
                except StopIteration:
                    pass
            live = going
        return carry
    lax.fori_loop(0, count // group, step, 0)


def flip(w):
    return w.astype(F32).T.astype(w.dtype)


def key_column(mask_row):
    return jnp.broadcast_to(mask_row, (128, mask_row.shape[1])).T


def project_row(r, x, mask_row, wt_ref, proj_s, keep_s):
    x_norm = yield from norm_steps(x)
    proj_s[r] = nt(wt_ref[...], x_norm).astype(BF16)
    keep_s[r] = key_column(mask_row)


def attend_rows(rows, proj_s, keep_s, gated_s, bias_ref, heads, group):
    width, length = gated_s.shape[1:]
    dim = width // heads

    def part(n, r, h):
        return proj_s[r, n * width + h * dim:n * width + (h + 1) * dim, :]

    def scores(r, h):
        logits = tn(part(1, r, h), part(0, r, h)) * (dim ** -0.5 * LOG2E)
        if bias_ref is not None:
            logits = logits + bias_ref[h]
        kept = jnp.concatenate([keep_s[r]] * (length // 128), axis=1) > 0
        return jnp.where(kept, logits, MASKED)

    def weigh(logits):
        expd = jnp.exp2(logits - jnp.max(logits, axis=0, keepdims=True))
        return (expd * (1.0 / jnp.sum(expd, axis=0, keepdims=True))).astype(BF16)

    def gate(r, h, probs):
        gated = nn(part(2, r, h), probs) * jax.nn.sigmoid(part(3, r, h).astype(F32))
        gated_s[r, h * dim:(h + 1) * dim, :] = gated.astype(BF16)

    def body(n):
        items = [(n * group + g, h) for g in range(group) for h in range(heads)]
        probs = None
        ahead = scores(*items[0])
        for k, item in enumerate(items):
            logits, ahead = ahead, scores(*items[k + 1]) if k + 1 < len(items) else None
            if probs is not None:
                gate(*items[k - 1], probs)
            probs = weigh(logits)
        gate(*items[-1], probs)
    each(rows // group, body)


def attention_scratch(rows, length, w, w_out):
    return [pltpu.VMEM((rows, w.shape[1], length), BF16), pltpu.VMEM((rows, length, 128), F32),
            pltpu.VMEM((rows, w_out.shape[0], length), BF16)]


def each(count, body, unroll=1):
    def step(n, carry):
        body(n)
        return carry
    lax.fori_loop(0, count, step, 0, unroll=unroll)


def load_bias(bias_ref, bias_s, transposed):
    for h in range(bias_s.shape[0]):
        bias = bias_ref[h].astype(F32) * LOG2E
        bias_s[h] = bias.T if transposed else bias


def transition_steps(x, w_in_ref, w_out_ref):
    x_norm = yield from norm_steps(x)
    hidden = jnp.maximum(nn(x_norm, w_in_ref[...]), 0.0).astype(BF16)
    yield
    update = nn(hidden, w_out_ref[...])
    yield
    return update


def residual(x, update):
    total = (x + update).astype(BF16)
    return total, total.astype(F32)


def rows_of(ref, start, count, step):
    return ref[pl.ds(start, count, stride=step), :]


def call(kernel, grid, in_specs, out_specs, out_shape, scratch, flops):
    return pl.pallas_call(
        kernel, grid=grid, in_specs=in_specs, out_specs=out_specs, out_shape=out_shape, scratch_shapes=scratch,
        compiler_params=pltpu.CompilerParams(vmem_limit_bytes=VMEM_LIMIT),
        cost_estimate=pl.CostEstimate(flops=flops, bytes_accessed=1 << 24, transcendentals=0))


def row_at(ref, n):
    if len(ref.shape) == 3:
        return ref[n]
    return jnp.concatenate([ref[d, n] for d in range(ref.shape[0])], axis=0)


def put_pieces(ref, n, value):
    size = ref.shape[2]
    for d in range(ref.shape[0]):
        ref[d, n] = value[d * size:(d + 1) * size]


def row_spec_of(x, block, first):
    if x.ndim == 3:
        return pl.BlockSpec((block,) + x.shape[1:], lambda n: (n + first, 0, 0))
    return pl.BlockSpec((x.shape[0], block) + x.shape[2:], lambda n: (0, n + first, 0, 0))


def full_spec(array):
    zeros = (0,) * array.ndim
    return pl.BlockSpec(array.shape, lambda n: zeros)


def lead_spec(block, axis):
    return pl.BlockSpec(block, lambda n: tuple(n if d == axis else 0 for d in range(len(block))))


def bias_rows(store, n, x_norm, wbt_ref):
    values = nt(wbt_ref[...], x_norm)
    for t in range(store.shape[0]):
        store[t, pl.ds(pl.multiple_of(n * 8, 8), 8), :] = values[:, t * 128:(t + 1) * 128]


def bias_scratch(rows, length):
    return pltpu.VMEM((length // 128, rows * 8, 128), F32)


def write_bias(out_ref, store, rows):
    for h in range(out_ref.shape[0]):
        out_ref[h] = take_row(store, h, rows, 8).astype(BF16)


def bias_kernel(z_ref, wbt_ref, out_ref, store):
    rows = z_ref.shape[0]

    def body(n, carry):
        bias_rows(store, n, norm(z_ref[n].astype(F32)), wbt_ref)
        return carry
    lax.fori_loop(0, rows, body, 0)
    write_bias(out_ref, store, rows)


def pair_bias(z, wbt, heads):
    rows, length, _ = z.shape
    return call(bias_kernel, (1,), [full_spec(z), full_spec(wbt)], lead_spec((heads, rows, length), 1),
                jax.ShapeDtypeStruct((heads, rows, length), BF16), [bias_scratch(rows, length)], 10 ** 8)(z, wbt)


def row_kernel(transposed, heads, m_ref, mask_ref, bias_ref, w_ref, w_out_ref, out_ref, bias_s, wt_s, proj_s, keep_s, gated_s):
    rows = mask_ref.shape[0]

    @pl.when(pl.program_id(0) == 0)
    def _():
        load_bias(bias_ref, bias_s, transposed)
        wt_s[...] = flip(w_ref[...])

    def project(s):
        yield from project_row(s, row_at(m_ref, s).astype(F32), mask_ref[pl.ds(s, 1), :], wt_s, proj_s, keep_s)
    together(rows, project, 2)
    attend_rows(rows, proj_s, keep_s, gated_s, bias_s, heads, 1)

    def finish(s):
        update = tn(gated_s[s], w_out_ref[...])
        yield
        put_pieces(out_ref, s, residual(row_at(m_ref, s).astype(F32), update)[0])
    together(rows, finish, 2)


def row_attention(m, mask, bias, transposed, w, w_out, pieces, part, parts):
    seqs, length = mask.shape
    chans = m.shape[-1]
    heads = bias.shape[0]
    block = 8
    steps = seqs // block // parts
    shape = (pieces, seqs // parts, length // pieces, chans)
    return call(functools.partial(row_kernel, transposed, heads), (steps,),
                [row_spec_of(m, block, part * steps), pl.BlockSpec((block, length), lambda n: (n + part * steps, 0)),
                 full_spec(bias), full_spec(w), full_spec(w_out)],
                lead_spec((pieces, block) + shape[2:], 1), jax.ShapeDtypeStruct(shape, BF16),
                [pltpu.VMEM((heads, length, length), F32), pltpu.VMEM(w.shape[::-1], BF16)] + attention_scratch(block, length, w, w_out),
                10 ** 10)(m, mask, bias, w, w_out)


def split_store(dst, parts):
    pieces, size, rows, chans = parts[0].shape
    for p, part in enumerate(parts):
        for d in range(pieces):
            flat = part[d].astype(F32).reshape(size * rows, chans)
            place = pl.ds((d * len(parts) + p) * size * rows, size * rows)
            for t in range(chans // 128):
                dst[t, place, :] = flat[:, t * 128:(t + 1) * 128]


def take_row(src, r, count, step):
    return jnp.concatenate([src[t, pl.ds(r, count, stride=step), :] for t in range(src.shape[0])], axis=1)


def put_row(dst, r, count, step, value):
    for t in range(dst.shape[0]):
        dst[t, pl.ds(r, count, stride=step), :] = value[:, t * 128:(t + 1) * 128]


def join_store(src, shape):
    seqs, rows, chans = shape
    return jnp.concatenate([src[t] for t in range(src.shape[0])], axis=1).reshape(seqs, rows, chans).astype(BF16)


def col_kernel(heads, parts, *refs):
    m_refs = refs[:parts]
    mask_ref, w_ref, w_out_ref, tin_ref, tout_ref, op_ref, out_ref, a_ref, b_ref, x_s, b_s, wt_s, opt_s, proj_s, keep_s, gated_s = refs[parts:]
    rows, seqs = mask_ref.shape
    chans = w_ref.shape[0]
    dim = op_ref.shape[1] // 2

    @pl.when(pl.program_id(0) == 0)
    def _():
        wt_s[...] = flip(w_ref[...])
        opt_s[...] = flip(op_ref[...])
    split_store(x_s, m_refs)

    def project(r):
        yield from project_row(r, take_row(x_s, r, seqs, rows), mask_ref[pl.ds(r, 1), :], wt_s, proj_s, keep_s)
    together(rows, project, 2)
    attend_rows(rows, proj_s, keep_s, gated_s, None, heads, 1)

    def finish(r):
        mask_row = mask_ref[pl.ds(r, 1), :]
        x = take_row(x_s, r, seqs, rows)
        update = tn(gated_s[r], w_out_ref[...])
        yield
        x = residual(x, update)[1]
        update = yield from transition_steps(x, tin_ref, tout_ref)
        x = residual(x, update)[1]
        x_norm = yield from norm_steps(x)
        proj = nt(opt_s[...], x_norm).astype(BF16).astype(F32) * mask_row
        yield
        put_row(x_s, r, seqs, rows, x)
        a_ref[r] = proj[:dim].astype(BF16)
        for t in range(seqs // 128):
            b_s[t, pl.ds(r, dim, stride=rows), :] = proj[dim:, t * 128:(t + 1) * 128]
    together(rows, finish, 2)
    out_ref[...] = join_store(x_s, (seqs, rows, chans)).reshape(out_ref.shape)
    b_ref[...] = join_store(b_s, b_ref.shape)


def column_block(m_parts, mask_t, heads, w, w_out, t_in, t_out, o_proj):
    rows, seqs = mask_t.shape
    pieces, size, _, chans = m_parts[0].shape
    parts = len(m_parts)
    dim = o_proj.shape[1] // 2
    block = 16
    weights = (w, w_out, t_in, t_out, o_proj)
    out_shape = (pieces, seqs // pieces, rows, chans)
    return call(functools.partial(col_kernel, heads, parts), (rows // block,),
                [lead_spec((pieces, size, block, chans), 2)] * parts + [lead_spec((block, seqs), 0)] + [full_spec(x) for x in weights],
                [lead_spec(out_shape[:2] + (block, chans), 2), lead_spec((block, dim, seqs), 0), lead_spec((dim, block, seqs), 1)],
                [jax.ShapeDtypeStruct(out_shape, BF16), jax.ShapeDtypeStruct((rows, dim, seqs), BF16), jax.ShapeDtypeStruct((dim, rows, seqs), BF16)],
                [pltpu.VMEM((chans // 128, seqs * block, 128), F32), pltpu.VMEM((seqs // 128, dim * block, 128), F32),
                 pltpu.VMEM(w.shape[::-1], BF16), pltpu.VMEM(o_proj.shape[::-1], BF16)] + attention_scratch(block, seqs, w, w_out),
                3 * 10 ** 10)(*m_parts, mask_t, *weights)


def gate_parts(z_norm, mask_row, wt_ref, tri):
    proj = nt(wt_ref[pl.ds(0, 4 * tri), :], z_norm)
    left = mask_row * jax.nn.sigmoid(proj[2 * tri:3 * tri]) * proj[:tri]
    right = mask_row * jax.nn.sigmoid(proj[3 * tri:]) * proj[tri:2 * tri]
    return left, right


def put_channels(dst, n, step, value):
    for t in range(dst.shape[0]):
        dst[t, pl.ds(n, value.shape[0], stride=step), :] = value[:, t * 128:(t + 1) * 128]


def opm_kernel(a_ref, b_ref, z_ref, rmask_ref, fmask_ref, pmask_ref, w_ref, proj_ref,
               z_out, l_out, r_out, wf_s, wt_s, gt_s, o_s, scale_s, l_s, r_s):
    rows, dim, seqs = a_ref.shape
    tri = l_out.shape[0]

    @pl.when(pl.program_id(0) == 0)
    def _():
        gt_s[...] = flip(proj_ref[...])
        wf_s[...] = w_ref[...].astype(F32)
        swapped = [rows_of(wf_s, e, dim, dim) for e in range(dim)]
        wt_s[...] = jnp.concatenate(swapped, axis=0).T.astype(BF16)
    scale_s[...] = 1.0 / (1e-3 + nt(rmask_ref[...].astype(BF16), fmask_ref[...].astype(BF16)))

    def outer(e, carry):
        prod = nt(a_ref[...].reshape(rows * dim, seqs), b_ref[e]).astype(BF16)
        for i in range(rows):
            o_s[i, pl.ds(pl.multiple_of(e * dim, dim), dim), :] = prod[i * dim:(i + 1) * dim]
        return carry
    lax.fori_loop(0, dim, outer, 0, unroll=2)

    def finish(i):
        update = nn(wt_s[...], o_s[i]) * scale_s[pl.ds(i, 1), :]
        yield
        total, total_f = residual(row_at(z_ref, i).astype(F32), update.T)
        yield
        z_norm = yield from norm_steps(total_f)
        left, right = gate_parts(z_norm, pmask_ref[pl.ds(i, 1), :], gt_s, tri)
        yield
        z_out[i] = total
        put_channels(l_s, i, rows, left)
        put_channels(r_s, i, rows, right)
    together(rows, finish, 2)
    l_out[...] = join_store(l_s, l_out.shape)
    r_out[...] = join_store(r_s, r_out.shape)


def outer_block(a, b_full, z, rmask, fmask, pmask, w_out, tri_proj, part, parts):
    rows, dim, seqs = a.shape
    length, out_dim = pmask.shape[1], z.shape[-1]
    tri = (tri_proj.shape[1] - out_dim) // 4
    block = rows // parts
    consts = (w_out, tri_proj)
    outs = [jax.ShapeDtypeStruct((block, length, out_dim), BF16)] + [jax.ShapeDtypeStruct((tri, block, length), BF16)] * 2
    chan_scratch = pltpu.VMEM((length // 128, tri * block, 128), F32)
    return call(opm_kernel, (1,),
                [pl.BlockSpec((block, dim, seqs), lambda n: (part, 0, 0)), full_spec(b_full), row_spec_of(z, block, part),
                 pl.BlockSpec((block, seqs), lambda n: (part, 0)), full_spec(fmask), pl.BlockSpec((block, length), lambda n: (part, 0))]
                + [full_spec(x) for x in consts], [full_spec(x) for x in outs], outs,
                [pltpu.VMEM(w_out.shape, F32), pltpu.VMEM(w_out.shape[::-1], BF16), pltpu.VMEM(tri_proj.shape[::-1], BF16),
                 pltpu.VMEM((block, dim * dim, length), BF16), pltpu.VMEM((block, length), F32), chan_scratch, chan_scratch],
                10 ** 10)(a, b_full, z, rmask, fmask, pmask, *consts)


def channel(b_refs, c, pieces):
    size = b_refs[0].shape[1] // pieces
    loaded = [ref[c] for ref in b_refs]
    return jnp.concatenate([x[d * size:(d + 1) * size] for d in range(pieces) for x in loaded], axis=0)


def put_product(x_s, c, rows, prod):
    for t in range(x_s.shape[0]):
        x_s[t, pl.ds(pl.multiple_of(c * rows, rows), rows), :] = prod[:, t * 128:(t + 1) * 128]


def tri_finish(x_s, z, i, rows, proj_ref, w_out_ref):
    out_dim = z.shape[1]
    chans = w_out_ref.shape[0]
    x = take_row(x_s, i, chans, rows)
    z_norm = yield from norm_steps(z)
    gate = nn(z_norm, proj_ref[:, 4 * chans:4 * chans + out_dim])
    centered = x - jnp.mean(x, axis=0, keepdims=True)
    variance = jnp.mean(centered * centered, axis=0, keepdims=True)
    x_norm = (centered * lax.rsqrt(variance + 1e-5)).astype(BF16)
    yield
    update = tn(x_norm, w_out_ref[...])
    gate = jax.nn.sigmoid(gate)
    yield
    return residual(z, gate * update)


def outgoing_kernel(parts, pieces, a_ref, *refs):
    b_refs = refs[:parts]
    z_ref, pmask_ref, proj_ref, w_out_ref, next_ref, z_out, l_out, r_out, x_s, r_s, gt_s = refs[parts:]
    step, steps = pl.program_id(0), pl.num_programs(0)
    block, rows, _ = a_ref.shape
    tri = w_out_ref.shape[0]

    def product(c, carry):
        put_product(x_s, step * block + c, rows, nt(a_ref[c], channel(b_refs, c, pieces)))
        return carry
    lax.fori_loop(0, block, product, 0, unroll=4)

    @pl.when(step == steps - 1)
    def _():
        gt_s[...] = flip(next_ref[...])

        def finish(i):
            mask_row = pmask_ref[pl.ds(i, 1), :]
            total, total_f = yield from tri_finish(x_s, z_ref[i].astype(F32), i, rows, proj_ref, w_out_ref)
            z_norm = yield from norm_steps(total_f)
            value = nn(z_norm, next_ref[:, :tri])
            value_gate = nn(z_norm, next_ref[:, 2 * tri:3 * tri])
            right = nt(gt_s[pl.ds(tri, tri), :], z_norm)
            right_gate = nt(gt_s[pl.ds(3 * tri, tri), :], z_norm)
            yield
            left = (key_column(mask_row) * jax.nn.sigmoid(value_gate) * value).astype(BF16)
            right = mask_row * jax.nn.sigmoid(right_gate) * right
            yield
            z_out[i] = total
            put_pieces(l_out, i, left)
            put_channels(r_s, i, rows, right)
        together(rows, finish, 2)
        r_out[...] = join_store(r_s, r_out.shape)


def outgoing(a, b_parts, z, pmask, proj, w_out, next_proj, pieces, part):
    tri, rows, length = a.shape
    block = 16
    parts = len(b_parts)
    weights = (proj, w_out, next_proj)
    scratch = pltpu.VMEM((length // 128, tri * rows, 128), F32)
    outs = [jax.ShapeDtypeStruct(z.shape, BF16), jax.ShapeDtypeStruct((pieces, rows, length // pieces, tri), BF16),
            jax.ShapeDtypeStruct((tri, rows, length), BF16)]
    return call(functools.partial(outgoing_kernel, parts, pieces), (tri // block,),
                [lead_spec((block, rows, length), 0)] + [lead_spec((block,) + x.shape[1:], 0) for x in b_parts]
                + [full_spec(z), pl.BlockSpec((rows, length), lambda n: (part, 0))] + [full_spec(x) for x in weights],
                [full_spec(x) for x in outs], outs, [scratch, scratch, pltpu.VMEM(next_proj.shape[::-1], BF16)],
                10 ** 10)(a, *b_parts, z, pmask, *weights)


def incoming_kernel(parts, *refs):
    a_refs, b_refs, z_refs = (refs[n * parts:(n + 1) * parts] for n in range(3))
    proj_ref, w_out_ref, wbt_ref, z_out, bias_out, af_s, a_s, x_s, bias_s = refs[3 * parts:]
    step, steps = pl.program_id(0), pl.num_programs(0)
    block = b_refs[0].shape[0]
    pieces, _, rows, tri = a_refs[0].shape
    length = z_out.shape[1]
    part_rows = z_refs[0].shape[0]

    @pl.when(step == 0)
    def _():
        split_store(af_s, a_refs)

        def turn(i):
            x = take_row(af_s, i, length, rows)
            yield
            put_channels(a_s, i, rows, x.T)
        together(rows, turn, 2)

    def product(c, carry):
        place = pl.ds(pl.multiple_of((step * block + c) * rows, rows), rows)
        left = jnp.concatenate([a_s[t, place, :] for t in range(a_s.shape[0])], axis=1).astype(BF16)
        put_product(x_s, step * block + c, rows, nn(left, channel(b_refs, c, pieces)))
        return carry
    lax.fori_loop(0, block, product, 0, unroll=4)

    @pl.when(step == steps - 1)
    def _():
        for p, z_ref in enumerate(z_refs):
            def finish(n, z_ref=z_ref, first=p * part_rows):
                i = first + n
                total, total_f = yield from tri_finish(x_s, z_ref[n].astype(F32), i, rows, proj_ref, w_out_ref)
                z_norm = yield from norm_steps(total_f)
                z_out[i] = total
                bias_rows(bias_s, i, z_norm, wbt_ref)
            together(part_rows, finish, 2)
        write_bias(bias_out, bias_s, rows)


def incoming(a_parts, b_parts, z_parts, proj, w_out, wbt, heads):
    pieces, _, rows, tri = a_parts[0].shape
    length, out_dim = z_parts[0].shape[1:]
    block = 16
    consts = (proj, w_out, wbt)
    scratch = pltpu.VMEM((length // 128, tri * rows, 128), F32)
    outs = [jax.ShapeDtypeStruct((rows, length, out_dim), BF16), jax.ShapeDtypeStruct((heads, rows, length), BF16)]
    return call(functools.partial(incoming_kernel, len(a_parts)), (tri // block,),
                [full_spec(x) for x in a_parts] + [lead_spec((block,) + x.shape[1:], 0) for x in b_parts] + [full_spec(x) for x in z_parts]
                + [full_spec(x) for x in consts], [full_spec(x) for x in outs], outs,
                [pltpu.VMEM((tri // 128, length * rows, 128), F32), scratch, scratch, bias_scratch(rows, length)],
                10 ** 10)(*a_parts, *b_parts, *z_parts, *consts)


def start_kernel(heads, z_ref, mask_ref, bias_ref, w_ref, w_out_ref, wbt_ref, z_out, bias_out, bias_s, wt_s, next_s, proj_s, keep_s, gated_s):
    rows = z_ref.shape[0]

    @pl.when(pl.program_id(0) == 0)
    def _():
        load_bias(bias_ref, bias_s, True)
        wt_s[...] = flip(w_ref[...])

    def project(i):
        yield from project_row(i, z_ref[i].astype(F32), mask_ref[pl.ds(i, 1), :], wt_s, proj_s, keep_s)
    together(rows, project, 4)
    attend_rows(rows, proj_s, keep_s, gated_s, bias_s, heads, 2)

    def finish(i):
        update = tn(gated_s[i], w_out_ref[...])
        yield
        total, total_f = residual(z_ref[i].astype(F32), update)
        z_norm = yield from norm_steps(total_f)
        put_pieces(z_out, i, total)
        bias_rows(next_s, i, z_norm, wbt_ref)
    together(rows, finish, 4)
    write_bias(bias_out, next_s, rows)


def start_attention(z, mask, bias, w, w_out, wbt, pieces, part, parts):
    rows, length, chans = z.shape
    heads = bias.shape[0]
    block = rows // parts
    consts = (bias, w, w_out, wbt)
    outs = [jax.ShapeDtypeStruct((pieces, block, length // pieces, chans), BF16), jax.ShapeDtypeStruct((heads, block, length), BF16)]
    return call(functools.partial(start_kernel, heads), (1,),
                [row_spec_of(z, block, part), pl.BlockSpec((block, length), lambda n: (part, 0))] + [full_spec(x) for x in consts],
                [full_spec(x) for x in outs], outs,
                [pltpu.VMEM((heads, length, length), F32), pltpu.VMEM(w.shape[::-1], BF16), bias_scratch(block, length)]
                + attention_scratch(block, length, w, w_out), 10 ** 10)(z, mask, *consts)


def end_kernel(heads, parts, *refs):
    z_refs = refs[:parts]
    mask_ref, bias_ref, w_ref, w_out_ref, tin_ref, tout_ref, wbt_ref, z_out, bias_out, x_s, bias_s, wt_s, next_s, proj_s, keep_s, gated_s = refs[parts:]
    cols, length = mask_ref.shape
    chans = w_ref.shape[0]

    @pl.when(pl.program_id(0) == 0)
    def _():
        load_bias(bias_ref, bias_s, False)
        wt_s[...] = flip(w_ref[...])
    split_store(x_s, z_refs)

    def project(j):
        yield from project_row(j, take_row(x_s, j, length, cols), mask_ref[pl.ds(j, 1), :], wt_s, proj_s, keep_s)
    together(cols, project, 4)
    attend_rows(cols, proj_s, keep_s, gated_s, bias_s, heads, 2)

    def finish(j):
        x = take_row(x_s, j, length, cols)
        update = tn(gated_s[j], w_out_ref[...])
        yield
        x = residual(x, update)[1]
        update = yield from transition_steps(x, tin_ref, tout_ref)
        x = residual(x, update)[1]
        x_norm = yield from norm_steps(x)
        put_row(x_s, j, length, cols, x)
        bias_rows(next_s, j, x_norm, wbt_ref)
    together(cols, finish, 2)
    z_out[...] = join_store(x_s, (length, cols, chans)).reshape(z_out.shape)
    write_bias(bias_out, next_s, cols)


def end_attention(z_parts, mask_t, bias, w, w_out, t_in, t_out, wbt, next_heads):
    cols, length = mask_t.shape
    pieces, size, _, chans = z_parts[0].shape
    parts = len(z_parts)
    heads = bias.shape[0]
    block = 16
    consts = (bias, w, w_out, t_in, t_out, wbt)
    out_shape = (pieces, length // pieces, cols, chans)
    return call(functools.partial(end_kernel, heads, parts), (cols // block,),
                [lead_spec((pieces, size, block, chans), 2)] * parts + [lead_spec((block, length), 0)] + [full_spec(x) for x in consts],
                [lead_spec(out_shape[:2] + (block, chans), 2), lead_spec((next_heads, block, length), 1)],
                [jax.ShapeDtypeStruct(out_shape, BF16), jax.ShapeDtypeStruct((next_heads, cols, length), BF16)],
                [pltpu.VMEM((chans // 128, length * block, 128), F32), pltpu.VMEM((heads, length, length), F32),
                 pltpu.VMEM(w.shape[::-1], BF16), bias_scratch(block, length)] + attention_scratch(block, length, w, w_out),
                10 ** 10)(*z_parts, mask_t, *consts)


def gather(x, axis):
    return lax.all_gather(x, GROUP_AXIS, axis=axis, tiled=True)


def exchange(x):
    return lax.all_to_all(x, GROUP_AXIS, 0, 0, tiled=True)


def rejoin(x):
    pieces, rows, size, chans = x.shape
    return jnp.swapaxes(x, 0, 1).reshape(rows, pieces * size, chans)


def bias_weight(w):
    return jnp.pad(w.T, ((0, 8 - w.shape[1]), (0, 0)))


def solution(mesh):
    row_spec = P((PARTS_AXIS, GROUP_AXIS))

    def local_body(m, z, msa_mask, pair_mask, *weights):
        layers = weights[0].shape[0]
        pieces, parts = mesh.shape[GROUP_AXIS], 2
        res_loc = z.shape[0]
        shard = lax.axis_index(GROUP_AXIS)
        heads = weights[1].shape[2]
        pair_heads = weights[14].shape[2]
        row_bias_w = [bias_weight(weights[1][n]) for n in range(layers)]
        seq_mask, row_mask = msa_mask.astype(F32), pair_mask.astype(F32)
        bias = pair_bias(z, row_bias_w[0], heads)
        packed = gather(jnp.concatenate([bias, msa_mask.astype(BF16)[None], pair_mask.astype(BF16)[None]]), 1)
        bias = packed[:heads]
        masks_t = jnp.swapaxes(packed[heads:].astype(F32), 1, 2)
        full_mask_t = masks_t[0]
        res_mask_t, col_mask = (lax.dynamic_slice_in_dim(x, shard * res_loc, res_loc, 0) for x in masks_t)
        for n in range(layers):
            (row_qkvg, _, row_out, col_qkvg, col_out, mtr_in, mtr_out, opm_proj, opm_out, tmo_proj, tmo_out, tmi_proj, tmi_out,
             tas_qkvg, tas_bias, tas_out, tae_qkvg, tae_bias, tae_out, ptr_in, ptr_out) = (weight[n] for weight in weights)
            m = [exchange(row_attention(m, seq_mask, bias, n == 0, row_qkvg, row_out, pieces, p, parts)) for p in range(parts)]
            m, left, right = column_block(m, res_mask_t, heads, col_qkvg, col_out, mtr_in, mtr_out, opm_proj)
            right = gather(right, 1)
            done = [outer_block(left, right, z, res_mask_t, full_mask_t, row_mask, opm_out, tmo_proj, p, parts) for p in range(parts)]
            full = [gather(x[2], 1) for x in done]
            done = [outgoing(x[1], full, x[0], row_mask, tmo_proj, tmo_out, tmi_proj, pieces, p) for p, x in enumerate(done)]
            left, full = [exchange(x[1]) for x in done], [gather(x[2], 1) for x in done]
            z, bias = incoming(left, full, [x[0] for x in done], tmi_proj, tmi_out, bias_weight(tas_bias), pair_heads)
            bias = gather(bias, 1)
            done = [start_attention(z, row_mask, bias, tas_qkvg, tas_out, bias_weight(tae_bias), pieces, p, parts) for p in range(parts)]
            z = [exchange(x[0]) for x in done]
            bias = gather(jnp.concatenate([x[1] for x in done], axis=1), 1)
            z, bias, m = lax.optimization_barrier((z, bias, m))
            m = exchange(m)
            z, bias = end_attention(z, col_mask, bias, tae_qkvg, tae_out, ptr_in, ptr_out, row_bias_w[min(n + 1, layers - 1)], heads)
            z, bias, m = lax.optimization_barrier((z, bias, m))
            if n < layers - 1:
                bias = gather(bias, 1)
            z = exchange(z)
        return rejoin(m), rejoin(z)

    def run_blocks(*arrays):
        n_weights = len(arrays) - 4
        return jax.shard_map(local_body, mesh=mesh, in_specs=(row_spec,) * 4 + (P(),) * n_weights, out_specs=(row_spec, row_spec), check_vma=False)(*arrays)

    return run_blocks
```

```python
import functools
import itertools
import math

import jax
import jax.numpy as jnp
from jax import lax
from jax.experimental import pallas as pl
from jax.experimental.pallas import tpu as pltpu
from jax.sharding import PartitionSpec as P

GROUP_AXIS = 'dap'
PARTS_AXIS = 'req'
LOG2E = math.log2(math.e)
MASKED = -1e9 * LOG2E
F32, BF16 = jnp.float32, jnp.bfloat16
VMEM_LIMIT = 60 * 1024 * 1024


def nn(a, b):
    return lax.dot_general(a, b, (((1,), (0,)), ((), ())), preferred_element_type=F32)


def nt(a, b):
    return lax.dot_general(a, b, (((1,), (1,)), ((), ())), preferred_element_type=F32)


def tn(a, b):
    return lax.dot_general(a, b, (((0,), (0,)), ((), ())), preferred_element_type=F32)


def norm(x):
    centered = x - jnp.mean(x, axis=-1, keepdims=True)
    variance = jnp.mean(centered * centered, axis=-1, keepdims=True)
    return (centered * lax.rsqrt(variance + 1e-5)).astype(BF16)


def norm_steps(x):
    centered = x - jnp.mean(x, axis=-1, keepdims=True)
    yield
    variance = jnp.mean(centered * centered, axis=-1, keepdims=True)
    yield
    return (centered * lax.rsqrt(variance + 1e-5)).astype(BF16)


def together(count, body, group):
    def step(n, carry):
        live = [body(n * group + g) for g in range(group)]
        while live:
            going = []
            for member in live:
                try:
                    next(member)
                    going.append(member)
                except StopIteration:
                    pass
            live = going
        return carry
    lax.fori_loop(0, count // group, step, 0)


def flip(w):
    return w.astype(F32).T.astype(w.dtype)


def key_column(mask_row):
    return jnp.broadcast_to(mask_row, (128, mask_row.shape[1])).T


def project_row(r, x, mask_row, wt_ref, proj_s, keep_s):
    x_norm = yield from norm_steps(x)
    proj_s[r] = nt(wt_ref[...], x_norm).astype(BF16)
    keep_s[r] = key_column(mask_row)


def attend_rows(rows, proj_s, keep_s, gated_s, bias_ref, heads, group):
    width, length = gated_s.shape[1:]
    dim = width // heads

    def part(n, r, h):
        return proj_s[r, n * width + h * dim:n * width + (h + 1) * dim, :]

    def scores(r, h):
        logits = tn(part(1, r, h), part(0, r, h)) * (dim ** -0.5 * LOG2E)
        if bias_ref is not None:
            logits = logits + bias_ref[h]
        kept = jnp.concatenate([keep_s[r]] * (length // 128), axis=1) > 0
        return jnp.where(kept, logits, MASKED)

    def weigh(logits):
        expd = jnp.exp2(logits - jnp.max(logits, axis=0, keepdims=True))
        return (expd * (1.0 / jnp.sum(expd, axis=0, keepdims=True))).astype(BF16)

    def gate(r, h, probs):
        gated = nn(part(2, r, h), probs) * jax.nn.sigmoid(part(3, r, h).astype(F32))
        gated_s[r, h * dim:(h + 1) * dim, :] = gated.astype(BF16)

    def body(n):
        items = [(n * group + g, h) for g in range(group) for h in range(heads)]
        probs = None
        ahead = scores(*items[0])
        for k, item in enumerate(items):
            logits, ahead = ahead, scores(*items[k + 1]) if k + 1 < len(items) else None
            if probs is not None:
                gate(*items[k - 1], probs)
            probs = weigh(logits)
        gate(*items[-1], probs)
    each(rows // group, body)


def attention_scratch(rows, length, w, w_out):
    return [pltpu.VMEM((rows, w.shape[1], length), BF16), pltpu.VMEM((rows, length, 128), F32),
            pltpu.VMEM((rows, w_out.shape[0], length), BF16)]


def each(count, body, unroll=1):
    def step(n, carry):
        body(n)
        return carry
    lax.fori_loop(0, count, step, 0, unroll=unroll)


def load_bias(bias_ref, bias_s, transposed):
    for h in range(bias_s.shape[0]):
        bias = bias_ref[h].astype(F32) * LOG2E
        bias_s[h] = bias.T if transposed else bias


def transition_steps(x, w_in_ref, w_out_ref):
    x_norm = yield from norm_steps(x)
    hidden = jnp.maximum(nn(x_norm, w_in_ref[...]), 0.0).astype(BF16)
    yield
    update = nn(hidden, w_out_ref[...])
    yield
    return update


def residual(x, update):
    total = (x + update).astype(BF16)
    return total, total.astype(F32)


def rows_of(ref, start, count, step):
    return ref[pl.ds(start, count, stride=step), :]


def call(kernel, grid, in_specs, out_specs, out_shape, scratch, flops):
    return pl.pallas_call(
        kernel, grid=grid, in_specs=in_specs, out_specs=out_specs, out_shape=out_shape, scratch_shapes=scratch,
        compiler_params=pltpu.CompilerParams(vmem_limit_bytes=VMEM_LIMIT),
        cost_estimate=pl.CostEstimate(flops=flops, bytes_accessed=1 << 24, transcendentals=0))


def row_at(ref, n):
    if len(ref.shape) == 3:
        return ref[n]
    return jnp.concatenate([ref[d, n] for d in range(ref.shape[0])], axis=0)


def put_pieces(ref, n, value):
    size = ref.shape[2]
    for d in range(ref.shape[0]):
        ref[d, n] = value[d * size:(d + 1) * size]


def row_spec_of(x, block, first):
    if x.ndim == 3:
        return pl.BlockSpec((block,) + x.shape[1:], lambda n: (n + first, 0, 0))
    return pl.BlockSpec((x.shape[0], block) + x.shape[2:], lambda n: (0, n + first, 0, 0))


def full_spec(array):
    zeros = (0,) * array.ndim
    return pl.BlockSpec(array.shape, lambda n: zeros)


def lead_spec(block, axis):
    return pl.BlockSpec(block, lambda n: tuple(n if d == axis else 0 for d in range(len(block))))


def bias_rows(store, n, x_norm, wbt_ref):
    values = nt(wbt_ref[...], x_norm)
    for t in range(store.shape[0]):
        store[t, pl.ds(pl.multiple_of(n * 8, 8), 8), :] = values[:, t * 128:(t + 1) * 128]


def bias_scratch(rows, length):
    return pltpu.VMEM((length // 128, rows * 8, 128), F32)


def write_bias(out_ref, store, rows):
    for h in range(out_ref.shape[0]):
        out_ref[h] = take_row(store, h, rows, 8).astype(BF16)


def bias_kernel(z_ref, wbt_ref, out_ref, store):
    rows = z_ref.shape[0]

    def body(n, carry):
        bias_rows(store, n, norm(z_ref[n].astype(F32)), wbt_ref)
        return carry
    lax.fori_loop(0, rows, body, 0)
    write_bias(out_ref, store, rows)


def pair_bias(z, wbt, heads):
    rows, length, _ = z.shape
    return call(bias_kernel, (1,), [full_spec(z), full_spec(wbt)], lead_spec((heads, rows, length), 1),
                jax.ShapeDtypeStruct((heads, rows, length), BF16), [bias_scratch(rows, length)], 10 ** 8)(z, wbt)


def row_kernel(transposed, heads, m_ref, mask_ref, bias_ref, w_ref, w_out_ref, out_ref, bias_s, wt_s, proj_s, keep_s, gated_s):
    rows = mask_ref.shape[0]

    @pl.when(pl.program_id(0) == 0)
    def _():
        load_bias(bias_ref, bias_s, transposed)
        wt_s[...] = flip(w_ref[...])

    def project(s):
        yield from project_row(s, row_at(m_ref, s).astype(F32), mask_ref[pl.ds(s, 1), :], wt_s, proj_s, keep_s)
    together(rows, project, 2)
    attend_rows(rows, proj_s, keep_s, gated_s, bias_s, heads, 1)

    def finish(s):
        update = tn(gated_s[s], w_out_ref[...])
        yield
        put_pieces(out_ref, s, residual(row_at(m_ref, s).astype(F32), update)[0])
    together(rows, finish, 2)


def row_attention(m, mask, bias, transposed, w, w_out, pieces, part, parts):
    seqs, length = mask.shape
    chans = m.shape[-1]
    heads = bias.shape[0]
    block = 8
    steps = seqs // block // parts
    shape = (pieces, seqs // parts, length // pieces, chans)
    return call(functools.partial(row_kernel, transposed, heads), (steps,),
                [row_spec_of(m, block, part * steps), pl.BlockSpec((block, length), lambda n: (n + part * steps, 0)),
                 full_spec(bias), full_spec(w), full_spec(w_out)],
                lead_spec((pieces, block) + shape[2:], 1), jax.ShapeDtypeStruct(shape, BF16),
                [pltpu.VMEM((heads, length, length), F32), pltpu.VMEM(w.shape[::-1], BF16)] + attention_scratch(block, length, w, w_out),
                10 ** 10)(m, mask, bias, w, w_out)


def split_store(dst, parts):
    pieces, size, rows, chans = parts[0].shape
    for p, part in enumerate(parts):
        for d in range(pieces):
            flat = part[d].astype(F32).reshape(size * rows, chans)
            place = pl.ds((d * len(parts) + p) * size * rows, size * rows)
            for t in range(chans // 128):
                dst[t, place, :] = flat[:, t * 128:(t + 1) * 128]


def take_row(src, r, count, step):
    return jnp.concatenate([src[t, pl.ds(r, count, stride=step), :] for t in range(src.shape[0])], axis=1)


def put_row(dst, r, count, step, value):
    for t in range(dst.shape[0]):
        dst[t, pl.ds(r, count, stride=step), :] = value[:, t * 128:(t + 1) * 128]


def join_store(src, shape):
    seqs, rows, chans = shape
    return jnp.concatenate([src[t] for t in range(src.shape[0])], axis=1).reshape(seqs, rows, chans).astype(BF16)


def col_kernel(heads, parts, held, *refs):
    m_refs, refs = refs[:parts], refs[held:]
    mask_ref, w_ref, w_out_ref, tin_ref, tout_ref, op_ref, out_ref, a_ref, b_ref, x_s, b_s, wt_s, opt_s, proj_s, keep_s, gated_s = refs[parts:]
    rows, seqs = mask_ref.shape
    chans = w_ref.shape[0]
    dim = op_ref.shape[1] // 2

    @pl.when(pl.program_id(0) == 0)
    def _():
        wt_s[...] = flip(w_ref[...])
        opt_s[...] = flip(op_ref[...])
    split_store(x_s, m_refs)

    def project(r):
        yield from project_row(r, take_row(x_s, r, seqs, rows), mask_ref[pl.ds(r, 1), :], wt_s, proj_s, keep_s)
    together(rows, project, 2)
    attend_rows(rows, proj_s, keep_s, gated_s, None, heads, 1)

    def finish(r):
        mask_row = mask_ref[pl.ds(r, 1), :]
        x = take_row(x_s, r, seqs, rows)
        update = tn(gated_s[r], w_out_ref[...])
        yield
        x = residual(x, update)[1]
        update = yield from transition_steps(x, tin_ref, tout_ref)
        x = residual(x, update)[1]
        x_norm = yield from norm_steps(x)
        proj = nt(opt_s[...], x_norm).astype(BF16).astype(F32) * mask_row
        yield
        put_row(x_s, r, seqs, rows, x)
        a_ref[r] = proj[:dim].astype(BF16)
        for t in range(seqs // 128):
            b_s[t, pl.ds(r, dim, stride=rows), :] = proj[dim:, t * 128:(t + 1) * 128]
    together(rows, finish, 2)
    out_ref[...] = join_store(x_s, (seqs, rows, chans)).reshape(out_ref.shape)
    b_ref[...] = join_store(b_s, b_ref.shape)


def column_block(m_parts, mask_t, heads, w, w_out, t_in, t_out, o_proj, part, parts, before):
    rows, seqs = mask_t.shape
    pieces, size, _, chans = m_parts[0].shape
    dim = o_proj.shape[1] // 2
    block = rows // parts
    weights = (w, w_out, t_in, t_out, o_proj)
    out_shape = (pieces, seqs // pieces, rows, chans)
    held = 0 if before is None else 1
    count = len(m_parts)
    return pl.pallas_call(
        functools.partial(col_kernel, heads, count, held), grid=(1,),
        in_specs=[pl.BlockSpec((pieces, size, block, chans), lambda n: (0, 0, part, 0))] * count + [pl.BlockSpec(memory_space=pl.ANY)] * held
        + [pl.BlockSpec((block, seqs), lambda n: (part, 0))] + [full_spec(x) for x in weights],
        out_specs=[pl.BlockSpec(out_shape[:2] + (block, chans), lambda n: (0, 0, part, 0)), lead_spec((block, dim, seqs), 0), lead_spec((dim, block, seqs), 0)],
        out_shape=[jax.ShapeDtypeStruct(out_shape, BF16), jax.ShapeDtypeStruct((block, dim, seqs), BF16), jax.ShapeDtypeStruct((dim, block, seqs), BF16)],
        scratch_shapes=[pltpu.VMEM((chans // 128, seqs * block, 128), F32), pltpu.VMEM((seqs // 128, dim * block, 128), F32),
                        pltpu.VMEM(w.shape[::-1], BF16), pltpu.VMEM(o_proj.shape[::-1], BF16)] + attention_scratch(block, seqs, w, w_out),
        input_output_aliases={count: 0} if held else {},
        compiler_params=pltpu.CompilerParams(vmem_limit_bytes=VMEM_LIMIT),
        cost_estimate=pl.CostEstimate(flops=15 * 10 ** 9, bytes_accessed=1 << 24, transcendentals=0),
    )(*m_parts, *([before] if held else []), mask_t, *weights)


def gate_parts(z_norm, mask_row, wt_ref, tri):
    proj = nt(wt_ref[pl.ds(0, 4 * tri), :], z_norm)
    left = mask_row * jax.nn.sigmoid(proj[2 * tri:3 * tri]) * proj[:tri]
    right = mask_row * jax.nn.sigmoid(proj[3 * tri:]) * proj[tri:2 * tri]
    return left, right


def put_channels(dst, n, step, value):
    for t in range(dst.shape[0]):
        dst[t, pl.ds(n, value.shape[0], stride=step), :] = value[:, t * 128:(t + 1) * 128]


def opm_kernel(parts, pieces, a_ref, *refs):
    b_refs = refs[:parts]
    (z_ref, rmask_ref, fmask_ref, pmask_ref, w_ref, proj_ref,
     z_out, l_out, r_out, wf_s, wt_s, gt_s, o_s, scale_s, l_s, r_s) = refs[parts:]
    rows, dim, seqs = a_ref.shape
    tri = l_out.shape[0]

    @pl.when(pl.program_id(0) == 0)
    def _():
        gt_s[...] = flip(proj_ref[...])
        wf_s[...] = w_ref[...].astype(F32)
        swapped = [rows_of(wf_s, e, dim, dim) for e in range(dim)]
        wt_s[...] = jnp.concatenate(swapped, axis=0).T.astype(BF16)
    scale_s[...] = 1.0 / (1e-3 + nt(rmask_ref[...].astype(BF16), fmask_ref[...].astype(BF16)))

    def outer(e, carry):
        prod = nt(a_ref[...].reshape(rows * dim, seqs), channel(b_refs, e, pieces)).astype(BF16)
        for i in range(rows):
            o_s[i, pl.ds(pl.multiple_of(e * dim, dim), dim), :] = prod[i * dim:(i + 1) * dim]
        return carry
    lax.fori_loop(0, dim, outer, 0, unroll=2)

    def finish(i):
        update = nn(wt_s[...], o_s[i]) * scale_s[pl.ds(i, 1), :]
        yield
        total, total_f = residual(row_at(z_ref, i).astype(F32), update.T)
        yield
        z_norm = yield from norm_steps(total_f)
        left, right = gate_parts(z_norm, pmask_ref[pl.ds(i, 1), :], gt_s, tri)
        yield
        z_out[i] = total
        put_channels(l_s, i, rows, left)
        put_channels(r_s, i, rows, right)
    together(rows, finish, 2)
    l_out[...] = join_store(l_s, l_out.shape)
    r_out[...] = join_store(r_s, r_out.shape)


def outer_block(a, b_parts, z, rmask, fmask, pmask, w_out, tri_proj, pieces, part):
    block, dim, seqs = a.shape
    length, out_dim = pmask.shape[1], z.shape[-1]
    tri = (tri_proj.shape[1] - out_dim) // 4
    consts = (w_out, tri_proj)
    outs = [jax.ShapeDtypeStruct((block, length, out_dim), BF16)] + [jax.ShapeDtypeStruct((tri, block, length), BF16)] * 2
    chan_scratch = pltpu.VMEM((length // 128, tri * block, 128), F32)
    return call(functools.partial(opm_kernel, len(b_parts), pieces), (1,),
                [full_spec(a)] + [full_spec(x) for x in b_parts] + [row_spec_of(z, block, part),
                 pl.BlockSpec((block, seqs), lambda n: (part, 0)), full_spec(fmask), pl.BlockSpec((block, length), lambda n: (part, 0))]
                + [full_spec(x) for x in consts], [full_spec(x) for x in outs], outs,
                [pltpu.VMEM(w_out.shape, F32), pltpu.VMEM(w_out.shape[::-1], BF16), pltpu.VMEM(tri_proj.shape[::-1], BF16),
                 pltpu.VMEM((block, dim * dim, length), BF16), pltpu.VMEM((block, length), F32), chan_scratch, chan_scratch],
                10 ** 10)(a, *b_parts, z, rmask, fmask, pmask, *consts)


def channel(b_refs, c, pieces):
    size = b_refs[0].shape[1] // pieces
    loaded = [ref[c] for ref in b_refs]
    return jnp.concatenate([x[d * size:(d + 1) * size] for d in range(pieces) for x in loaded], axis=0)


def put_product(x_s, c, rows, prod):
    for t in range(x_s.shape[0]):
        x_s[t, pl.ds(pl.multiple_of(c * rows, rows), rows), :] = prod[:, t * 128:(t + 1) * 128]


def tri_finish(x_s, z, i, rows, proj_ref, w_out_ref):
    out_dim = z.shape[1]
    chans = w_out_ref.shape[0]
    x = take_row(x_s, i, chans, rows)
    z_norm = yield from norm_steps(z)
    gate = nn(z_norm, proj_ref[:, 4 * chans:4 * chans + out_dim])
    centered = x - jnp.mean(x, axis=0, keepdims=True)
    variance = jnp.mean(centered * centered, axis=0, keepdims=True)
    x_norm = (centered * lax.rsqrt(variance + 1e-5)).astype(BF16)
    yield
    update = tn(x_norm, w_out_ref[...])
    gate = jax.nn.sigmoid(gate)
    yield
    return residual(z, gate * update)


def outgoing_kernel(parts, pieces, a_ref, *refs):
    b_refs = refs[:parts]
    z_ref, pmask_ref, proj_ref, w_out_ref, next_ref, z_out, l_out, r_out, x_s, r_s, gt_s = refs[parts:]
    step, steps = pl.program_id(0), pl.num_programs(0)
    block, rows, _ = a_ref.shape
    tri = w_out_ref.shape[0]

    def product(c, carry):
        put_product(x_s, step * block + c, rows, nt(a_ref[c], channel(b_refs, c, pieces)))
        return carry
    lax.fori_loop(0, block, product, 0, unroll=4)

    @pl.when(step == steps - 1)
    def _():
        gt_s[...] = flip(next_ref[...])

        def finish(i):
            mask_row = pmask_ref[pl.ds(i, 1), :]
            total, total_f = yield from tri_finish(x_s, z_ref[i].astype(F32), i, rows, proj_ref, w_out_ref)
            z_norm = yield from norm_steps(total_f)
            value = nn(z_norm, next_ref[:, :tri])
            value_gate = nn(z_norm, next_ref[:, 2 * tri:3 * tri])
            right = nt(gt_s[pl.ds(tri, tri), :], z_norm)
            right_gate = nt(gt_s[pl.ds(3 * tri, tri), :], z_norm)
            yield
            left = (key_column(mask_row) * jax.nn.sigmoid(value_gate) * value).astype(BF16)
            right = mask_row * jax.nn.sigmoid(right_gate) * right
            yield
            z_out[i] = total
            put_pieces(l_out, i, left)
            put_channels(r_s, i, rows, right)
        together(rows, finish, 2)
        r_out[...] = join_store(r_s, r_out.shape)


def outgoing(a, b_parts, z, pmask, proj, w_out, next_proj, pieces, part):
    tri, rows, length = a.shape
    block = 16
    parts = len(b_parts)
    weights = (proj, w_out, next_proj)
    scratch = pltpu.VMEM((length // 128, tri * rows, 128), F32)
    outs = [jax.ShapeDtypeStruct(z.shape, BF16), jax.ShapeDtypeStruct((pieces, rows, length // pieces, tri), BF16),
            jax.ShapeDtypeStruct((tri, rows, length), BF16)]
    return call(functools.partial(outgoing_kernel, parts, pieces), (tri // block,),
                [lead_spec((block, rows, length), 0)] + [lead_spec((block,) + x.shape[1:], 0) for x in b_parts]
                + [full_spec(z), pl.BlockSpec((rows, length), lambda n: (part, 0))] + [full_spec(x) for x in weights],
                [full_spec(x) for x in outs], outs, [scratch, scratch, pltpu.VMEM(next_proj.shape[::-1], BF16)],
                10 ** 10)(a, *b_parts, z, pmask, *weights)


def incoming_kernel(parts, *refs):
    a_refs, b_refs, z_refs = (refs[n * parts:(n + 1) * parts] for n in range(3))
    proj_ref, w_out_ref, wbt_ref, z_out, bias_out, af_s, a_s, x_s, bias_s = refs[3 * parts:]
    step, steps = pl.program_id(0), pl.num_programs(0)
    block = b_refs[0].shape[0]
    pieces, _, rows, tri = a_refs[0].shape
    length = z_out.shape[1]
    part_rows = z_refs[0].shape[0]

    @pl.when(step == 0)
    def _():
        split_store(af_s, a_refs)

        def turn(i):
            x = take_row(af_s, i, length, rows)
            yield
            put_channels(a_s, i, rows, x.T)
        together(rows, turn, 2)

    def product(c, carry):
        place = pl.ds(pl.multiple_of((step * block + c) * rows, rows), rows)
        left = jnp.concatenate([a_s[t, place, :] for t in range(a_s.shape[0])], axis=1).astype(BF16)
        put_product(x_s, step * block + c, rows, nn(left, channel(b_refs, c, pieces)))
        return carry
    lax.fori_loop(0, block, product, 0, unroll=4)

    @pl.when(step == steps - 1)
    def _():
        for p, z_ref in enumerate(z_refs):
            def finish(n, z_ref=z_ref, first=p * part_rows):
                i = first + n
                total, total_f = yield from tri_finish(x_s, z_ref[n].astype(F32), i, rows, proj_ref, w_out_ref)
                z_norm = yield from norm_steps(total_f)
                z_out[i] = total
                bias_rows(bias_s, i, z_norm, wbt_ref)
            together(part_rows, finish, 2)
        write_bias(bias_out, bias_s, rows)


def incoming(a_parts, b_parts, z_parts, proj, w_out, wbt, heads):
    pieces, _, rows, tri = a_parts[0].shape
    length, out_dim = z_parts[0].shape[1:]
    block = 16
    consts = (proj, w_out, wbt)
    scratch = pltpu.VMEM((length // 128, tri * rows, 128), F32)
    outs = [jax.ShapeDtypeStruct((rows, length, out_dim), BF16), jax.ShapeDtypeStruct((heads, rows, length), BF16)]
    return call(functools.partial(incoming_kernel, len(a_parts)), (tri // block,),
                [full_spec(x) for x in a_parts] + [lead_spec((block,) + x.shape[1:], 0) for x in b_parts] + [full_spec(x) for x in z_parts]
                + [full_spec(x) for x in consts], [full_spec(x) for x in outs], outs,
                [pltpu.VMEM((tri // 128, length * rows, 128), F32), scratch, scratch, bias_scratch(rows, length)],
                10 ** 10)(*a_parts, *b_parts, *z_parts, *consts)


def start_kernel(heads, z_ref, mask_ref, bias_ref, w_ref, w_out_ref, wbt_ref, z_out, bias_out, bias_s, wt_s, next_s, proj_s, keep_s, gated_s):
    rows = z_ref.shape[0]

    @pl.when(pl.program_id(0) == 0)
    def _():
        load_bias(bias_ref, bias_s, True)
        wt_s[...] = flip(w_ref[...])

    def project(i):
        yield from project_row(i, z_ref[i].astype(F32), mask_ref[pl.ds(i, 1), :], wt_s, proj_s, keep_s)
    together(rows, project, 4)
    attend_rows(rows, proj_s, keep_s, gated_s, bias_s, heads, 2)

    def finish(i):
        update = tn(gated_s[i], w_out_ref[...])
        yield
        total, total_f = residual(z_ref[i].astype(F32), update)
        z_norm = yield from norm_steps(total_f)
        put_pieces(z_out, i, total)
        bias_rows(next_s, i, z_norm, wbt_ref)
    together(rows, finish, 4)
    write_bias(bias_out, next_s, rows)


def start_attention(z, mask, bias, w, w_out, wbt, pieces, part, parts):
    rows, length, chans = z.shape
    heads = bias.shape[0]
    block = rows // parts
    consts = (bias, w, w_out, wbt)
    outs = [jax.ShapeDtypeStruct((pieces, block, length // pieces, chans), BF16), jax.ShapeDtypeStruct((heads, block, length), BF16)]
    return call(functools.partial(start_kernel, heads), (1,),
                [row_spec_of(z, block, part), pl.BlockSpec((block, length), lambda n: (part, 0))] + [full_spec(x) for x in consts],
                [full_spec(x) for x in outs], outs,
                [pltpu.VMEM((heads, length, length), F32), pltpu.VMEM(w.shape[::-1], BF16), bias_scratch(block, length)]
                + attention_scratch(block, length, w, w_out), 10 ** 10)(z, mask, *consts)


def end_kernel(heads, parts, *refs):
    z_refs = refs[:parts]
    mask_ref, bias_ref, w_ref, w_out_ref, tin_ref, tout_ref, wbt_ref, z_out, bias_out, x_s, bias_s, wt_s, next_s, proj_s, keep_s, gated_s = refs[parts:]
    cols, length = mask_ref.shape
    chans = w_ref.shape[0]

    @pl.when(pl.program_id(0) == 0)
    def _():
        load_bias(bias_ref, bias_s, False)
        wt_s[...] = flip(w_ref[...])
    split_store(x_s, z_refs)

    def project(j):
        yield from project_row(j, take_row(x_s, j, length, cols), mask_ref[pl.ds(j, 1), :], wt_s, proj_s, keep_s)
    together(cols, project, 4)
    attend_rows(cols, proj_s, keep_s, gated_s, bias_s, heads, 2)

    def finish(j):
        x = take_row(x_s, j, length, cols)
        update = tn(gated_s[j], w_out_ref[...])
        yield
        x = residual(x, update)[1]
        update = yield from transition_steps(x, tin_ref, tout_ref)
        x = residual(x, update)[1]
        x_norm = yield from norm_steps(x)
        put_row(x_s, j, length, cols, x)
        bias_rows(next_s, j, x_norm, wbt_ref)
    together(cols, finish, 2)
    z_out[...] = join_store(x_s, (length, cols, chans)).reshape(z_out.shape)
    write_bias(bias_out, next_s, cols)


def end_attention(z_parts, mask_t, bias, w, w_out, t_in, t_out, wbt, next_heads):
    cols, length = mask_t.shape
    pieces, size, _, chans = z_parts[0].shape
    parts = len(z_parts)
    heads = bias.shape[0]
    block = 16
    consts = (bias, w, w_out, t_in, t_out, wbt)
    out_shape = (pieces, length // pieces, cols, chans)
    return call(functools.partial(end_kernel, heads, parts), (cols // block,),
                [lead_spec((pieces, size, block, chans), 2)] * parts + [lead_spec((block, length), 0)] + [full_spec(x) for x in consts],
                [lead_spec(out_shape[:2] + (block, chans), 2), lead_spec((next_heads, block, length), 1)],
                [jax.ShapeDtypeStruct(out_shape, BF16), jax.ShapeDtypeStruct((next_heads, cols, length), BF16)],
                [pltpu.VMEM((chans // 128, length * block, 128), F32), pltpu.VMEM((heads, length, length), F32),
                 pltpu.VMEM(w.shape[::-1], BF16), bias_scratch(block, length)] + attention_scratch(block, length, w, w_out),
                10 ** 10)(*z_parts, mask_t, *consts)


def gather(x, axis):
    return lax.all_gather(x, GROUP_AXIS, axis=axis, tiled=True)


def exchange(x):
    return lax.all_to_all(x, GROUP_AXIS, 0, 0, tiled=True)


def rejoin(x):
    pieces, rows, size, chans = x.shape
    return jnp.swapaxes(x, 0, 1).reshape(rows, pieces * size, chans)


def spread_kernel(count, x_ref, out_ref, own_sem, send_sem, recv_sem, mate_send, mate_recv):
    me = lax.axis_index(GROUP_AXIS)
    rows = x_ref.shape[1]
    mate = me + 1 - 2 * lax.rem(me, 2)
    hops = [2 * k for k in range(1, count // 2)]

    barrier = pltpu.get_barrier_semaphore()
    for other in [lax.rem(me + hop, count) for hop in hops] + [mate]:
        pl.semaphore_signal(barrier, inc=1, device_id={GROUP_AXIS: other}, device_id_type=pl.DeviceIdType.MESH)
    pl.semaphore_wait(barrier, len(hops) + 1)

    def place(owner):
        return out_ref.at[:, pl.ds(pl.multiple_of(owner * rows, rows), rows), :]

    def send(src, owner, send_at, recv_at, target):
        copy = pltpu.make_async_remote_copy(src_ref=src, dst_ref=place(owner), send_sem=send_at, recv_sem=recv_at,
                                            device_id={GROUP_AXIS: target}, device_id_type=pl.DeviceIdType.MESH)
        copy.start()
        return copy

    far = [send(x_ref, me, send_sem.at[k], recv_sem.at[k], lax.rem(me + hop, count)) for k, hop in enumerate(hops)]
    near = [send(x_ref, me, mate_send.at[len(hops)], mate_recv.at[len(hops)], mate)]
    own = pltpu.make_async_copy(x_ref, place(me), own_sem)
    own.start()
    for k, hop in enumerate(hops):
        far[k].wait_recv()
        owner = lax.rem(me + count - hop, count)
        near.append(send(place(owner), owner, mate_send.at[k], mate_recv.at[k], mate))
    own.wait()
    for copy in far:
        copy.wait_send()
    for copy in near:
        copy.wait()


def spread_call(x, count, ident):
    heads, rows, length = x.shape
    hops = count // 2 - 1
    return pl.pallas_call(
        functools.partial(spread_kernel, count), out_shape=jax.ShapeDtypeStruct((heads, rows * count, length), x.dtype),
        in_specs=[pl.BlockSpec(memory_space=pltpu.VMEM)], out_specs=pl.BlockSpec(memory_space=pltpu.VMEM),
        scratch_shapes=[pltpu.SemaphoreType.DMA, pltpu.SemaphoreType.DMA((hops,)), pltpu.SemaphoreType.DMA((hops,)),
                        pltpu.SemaphoreType.DMA((hops + 1,)), pltpu.SemaphoreType.DMA((hops + 1,))],
        compiler_params=pltpu.CompilerParams(collective_id=ident, has_side_effects=True),
        cost_estimate=pl.CostEstimate(flops=10 ** 8, bytes_accessed=1 << 21, transcendentals=0))(x)


def bias_weight(w):
    return jnp.pad(w.T, ((0, 8 - w.shape[1]), (0, 0)))


def solution(mesh):
    row_spec = P((PARTS_AXIS, GROUP_AXIS))

    def local_body(m, z, msa_mask, pair_mask, *weights):
        layers = weights[0].shape[0]
        pieces, parts = mesh.shape[GROUP_AXIS], 2
        idents = itertools.count()

        def spread(x):
            return spread_call(x, pieces, next(idents))
        res_loc = z.shape[0]
        shard = lax.axis_index(GROUP_AXIS)
        heads = weights[1].shape[2]
        pair_heads = weights[14].shape[2]
        row_bias_w = [bias_weight(weights[1][n]) for n in range(layers)]
        seq_mask, row_mask = msa_mask.astype(F32), pair_mask.astype(F32)
        bias = pair_bias(z, row_bias_w[0], heads)
        packed = spread(jnp.concatenate([bias, msa_mask.astype(BF16)[None], pair_mask.astype(BF16)[None]]))
        bias = packed[:heads]
        masks_t = jnp.swapaxes(packed[heads:].astype(F32), 1, 2)
        full_mask_t = masks_t[0]
        res_mask_t, col_mask = (lax.dynamic_slice_in_dim(x, shard * res_loc, res_loc, 0) for x in masks_t)
        for n in range(layers):
            (row_qkvg, _, row_out, col_qkvg, col_out, mtr_in, mtr_out, opm_proj, opm_out, tmo_proj, tmo_out, tmi_proj, tmi_out,
             tas_qkvg, tas_bias, tas_out, tae_qkvg, tae_bias, tae_out, ptr_in, ptr_out) = (weight[n] for weight in weights)
            rows = [row_attention(m, seq_mask, bias, n == 0, row_qkvg, row_out, pieces, p, parts) for p in range(parts)]
            if n > 0:
                rows[0], z = lax.optimization_barrier((rows[0], z))
            rows = [exchange(x) for x in rows]
            m, left, right = None, [], []
            for p in range(parts):
                m, a_part, b_part = column_block(rows, res_mask_t, heads, col_qkvg, col_out, mtr_in, mtr_out, opm_proj, p, parts, m)
                left.append(a_part)
                right.append(gather(b_part, 1))
            done = [outer_block(left[p], right, z, res_mask_t, full_mask_t, row_mask, opm_out, tmo_proj, pieces, p) for p in range(parts)]
            full = [gather(x[2], 1) for x in done]
            done = [outgoing(x[1], full, x[0], row_mask, tmo_proj, tmo_out, tmi_proj, pieces, p) for p, x in enumerate(done)]
            left, full = [exchange(x[1]) for x in done], [gather(x[2], 1) for x in done]
            z, bias = incoming(left, full, [x[0] for x in done], tmi_proj, tmi_out, bias_weight(tas_bias), pair_heads)
            bias = spread(bias)
            done = [start_attention(z, row_mask, bias, tas_qkvg, tas_out, bias_weight(tae_bias), pieces, p, parts) for p in range(parts)]
            z = [exchange(x[0]) for x in done]
            bias = spread(jnp.concatenate([x[1] for x in done], axis=1))
            z, bias, m = lax.optimization_barrier((z, bias, m))
            m = exchange(m)
            z, bias = end_attention(z, col_mask, bias, tae_qkvg, tae_out, ptr_in, ptr_out, row_bias_w[min(n + 1, layers - 1)], heads)
            z, bias, m = lax.optimization_barrier((z, bias, m))
            if n < layers - 1:
                bias, z = lax.optimization_barrier((spread(bias), z))
            z = exchange(z)
        return rejoin(m), rejoin(z)

    def run_blocks(*arrays):
        n_weights = len(arrays) - 4
        return jax.shard_map(local_body, mesh=mesh, in_specs=(row_spec,) * 4 + (P(),) * n_weights, out_specs=(row_spec, row_spec), check_vma=False)(*arrays)

    return run_blocks
```
